128 devices in a mesh: gx: 4 (over z), gy: 4 (over y), gz: 8 (over x, core).
Axes of the slice: x: 4, y: 4, z: 4, core: 2. Of those that a mesh axis runs over, the one named last changes fastest.
Arguments:
- test_vectors: float32 [8, 64, 64, 8192], P(None, 'gx', 'gy', 'gz'), as said below
- aniso: int32 [3, 2], replicated, may hold values from 2 to 4
Outputs:
- basis: float32 [8, 64, 64, 8192], P(None, 'gx', 'gy', 'gz')
- coarse_basis: float32 [8, 32, 32, 4096], P(None, 'gx', 'gy', 'gz')
The draws below stay inside these ranges and needn't reach their ends.
Inputs may be any that keep to these rules, and one draw needn't show every extreme that they name: `test_vectors`: positive and negative values; every test vector is linearly independent of the others.
All inputs are finite; a program needn't handle non-finite values.
Results may differ from the reference program's by a relative error of at most 0.00029.
Values sent between devices are 32-bit elements; how exact they have to be, the bound alone decides.
A program may use at most 384 MiB of HBM per device.

```python
import jax
import jax.numpy as jnp
from jax import lax

K = 8
SWEEPS = 3
NX = 64
NY = 64
NZ = 8192


def draw_test_vectors(key, part):
    key_noise = jax.random.fold_in(key, 11)
    key_cells = jax.random.fold_in(key, 12)
    key_vectors = jax.random.fold_in(key, 13)
    key_blocks = jax.random.fold_in(key, 15)
    full_shape = (K, NX, NY, NZ)
    grid_shape = (1, NX, NY, NZ)
    index_x = lax.broadcasted_iota(jnp.float32, grid_shape, 1) / NX
    index_y = lax.broadcasted_iota(jnp.float32, grid_shape, 2) / NY
    index_z = lax.broadcasted_iota(jnp.float32, grid_shape, 3) / NZ
    position = (index_x + index_y + index_z) / 3.0
    values = jax.random.normal(key_noise, full_shape, jnp.float32)
    envelope = jnp.exp(jnp.log(3.0) * position)
    cell_scale = jnp.exp(jax.random.uniform(key_cells, grid_shape, jnp.float32, 0.0, jnp.log(10.0)))
    vector_scale = jnp.exp(jax.random.uniform(key_vectors, (K, 1, 1, 1), jnp.float32, 0.0, jnp.log(10.0)))
    block_table = jnp.exp(jax.random.uniform(key_blocks, (K, 2, 2, 2), jnp.float32, 0.0, jnp.log(10.0)))
    block_x = lax.broadcasted_iota(jnp.int32, (NX, 1, 1), 0) * 2 // NX
    block_y = lax.broadcasted_iota(jnp.int32, (1, NY, 1), 1) * 2 // NY
    block_z = lax.broadcasted_iota(jnp.int32, (1, 1, NZ), 2) * 2 // NZ
    block_scale = block_table[:, block_x, block_y, block_z]
    return values * cell_scale * vector_scale * block_scale * envelope


def set_ends(array, key, least, top_value):
    longest = array.shape.index(max(array.shape))
    spots = []
    for shift in (0, 1):
        where = [jax.random.randint(jax.random.fold_in(key, axis), (), 0, length) for axis, length in enumerate(array.shape)]
        where[longest] = (where[longest] + shift) % array.shape[longest]
        spots.append(tuple(where))
    return array.at[spots[0]].set(least).at[spots[1]].set(top_value)


def setup_inputs(seed: int = 0) -> dict:
    splits = jax.random.split(jax.random.key(seed), 3)
    return {
        "test_vectors": draw_test_vectors(jax.random.fold_in(splits[2], 71), 0),
        "aniso": set_ends(jax.random.randint(splits[1], (3, 2), 2, 5), jax.random.fold_in(splits[1], 1), 2, 4).astype(jnp.int32),
    }


omega_weight = 2.0 / 3.0

def jacobi_sweep(fields, coefficients, scaled):
    padded = jnp.pad(fields, ((0, 0), (1, 1), (1, 1), (1, 1)))
    center = padded[:, 1:-1, 1:-1, 1:-1]
    beside = coefficients[0] * (padded[:, 2:, 1:-1, 1:-1] + padded[:, :-2, 1:-1, 1:-1])
    beside = beside + coefficients[1] * (padded[:, 1:-1, 2:, 1:-1] + padded[:, 1:-1, :-2, 1:-1])
    beside = beside + coefficients[2] * (padded[:, 1:-1, 1:-1, 2:] + padded[:, 1:-1, 1:-1, :-2])
    return (1.0 - omega_weight) * center + scaled * beside

def orthonormal(gram_total, data):
    lower_factor = jnp.linalg.cholesky(gram_total)
    eye_matrix = jnp.eye(gram_total.shape[0], dtype=gram_total.dtype)
    inverse = jax.scipy.linalg.solve_triangular(lower_factor, eye_matrix, lower=True)
    return jnp.einsum('kl,lxyz->kxyz', inverse, data, precision=lax.Precision.HIGHEST)

def reference(test_vectors, aniso):
    coefficients = aniso[:, 0].astype(jnp.float32) / aniso[:, 1].astype(jnp.float32)
    scaled = omega_weight / (2.0 * (coefficients[0] + coefficients[1] + coefficients[2]))
    fields = test_vectors
    for sweep_index in range(SWEEPS):
        fields = jacobi_sweep(fields, coefficients, scaled)
    flattened = fields.reshape(K, -1)
    cell_count = NX * NY * NZ
    gram_total = jnp.dot(flattened, flattened.T, precision=lax.Precision.HIGHEST) / cell_count
    coarse = fields.reshape(K, NX // 2, 2, NY // 2, 2, NZ // 2, 2).mean(axis=(2, 4, 6))
    coarse_flat = coarse.reshape(K, -1)
    coarse_gram = jnp.dot(coarse_flat, coarse_flat.T, precision=lax.Precision.HIGHEST) / (cell_count // 8)
    return (orthonormal(gram_total, fields), orthonormal(coarse_gram, coarse))
```

```python
import functools

import jax
import jax.numpy as jnp
from jax import lax
from jax.experimental import pallas as pl
from jax.experimental.pallas import tpu as pltpu
from jax.sharding import PartitionSpec as P

MESH = pl.DeviceIdType.MESH
omega_weight = 2.0 / 3.0
K = 8
SWEEPS = 3
LANES = 128
AXES = ("gx", "gy", "gz")


def sweep_kernel(
    sizes,
    aniso_ref,
    in_ref,
    fields_ref,
    coarse_ref,
    gram_ref,
    state,
    ysend,
    yrecv,
    pairs,
    quarter,
    fine_acc,
    coarse_acc,
    gather_z,
    gather_y,
    gather_x,
    load_sem,
    send_sem,
    recv_sem,
    gsend_sem,
    grecv_sem,
):
    rows_x, rows_y, blocks = (in_ref.shape[1], in_ref.shape[2], in_ref.shape[3] // LANES)
    area = blocks * rows_y
    position = {axis: lax.axis_index(axis) for axis in AXES}

    def load(k, block):
        return pltpu.make_async_copy(
            in_ref.at[k, :, :, pl.ds(block * LANES, LANES)],
            state.at[0, k, pl.ds(1, rows_x), pl.ds((block + 1) * rows_y, rows_y), :],
            load_sem.at[k, block],
        )

    def start_loads(k, carry):
        for block in range(blocks):
            load(k, block).start()
        return carry

    lax.fori_loop(0, K, start_loads, 0)

    barrier = pltpu.get_barrier_semaphore()
    peers = 0
    for axis in AXES:
        for offset in range(1, sizes[axis]):
            peer = lax.rem(position[axis] + offset, sizes[axis])
            pl.semaphore_signal(barrier, inc=1, device_id={axis: peer}, device_id_type=MESH)
            peers += 1

    def as_float(d, j):
        return jnp.full((8, LANES), aniso_ref[d, j], jnp.int32).astype(jnp.float32)

    coefficients = [as_float(d, 0) / as_float(d, 1) for d in range(3)]
    scaled = omega_weight / (2.0 * (coefficients[0] + coefficients[1] + coefficients[2]))
    weights = [scaled * c for c in coefficients]
    keep = 1.0 - omega_weight

    lane = lax.broadcasted_iota(jnp.int32, (8, LANES), 1)
    row = lax.broadcasted_iota(jnp.int32, (8, LANES), 0)

    def face(s, k, direction):
        b = s % 2
        axis, side = AXES[direction // 2], direction % 2
        peer = position[axis] + (1 if side else -1)
        if axis == "gx":
            source = state.at[b, k, rows_x if side else 1, pl.ds(rows_y, area), :]
            target = state.at[b, k, 0 if side else rows_x + 1, pl.ds(rows_y, area), :]
        elif axis == "gy":
            source = ysend.at[s, side, k]
            target = yrecv.at[s, side, k]
        else:
            from_row = blocks * rows_y if side else rows_y
            to_row = 0 if side else (blocks + 1) * rows_y
            source = state.at[b, k, pl.ds(1, rows_x), pl.ds(from_row, rows_y), :]
            target = state.at[b, k, pl.ds(1, rows_x), pl.ds(to_row, rows_y), :]
        return pltpu.make_async_remote_copy(
            src_ref=source,
            dst_ref=target,
            send_sem=send_sem.at[direction, s, k],
            recv_sem=recv_sem.at[direction, s, k],
            device_id={axis: peer},
            device_id_type=MESH,
        )

    def can_send(direction):
        axis, side = AXES[direction // 2], direction % 2
        return position[axis] < sizes[axis] - 1 if side else position[axis] > 0

    def can_receive(direction):
        return can_send(direction ^ 1)

    def send(s, k):
        b = s % 2

        def pack(x, carry):
            for side in range(2):
                first = rows_y + (rows_y - 1 if side else 0)
                ysend[s, side, k, x] = state[b, k, x + 1, pl.ds(first, blocks, stride=rows_y), :]
            return carry

        lax.fori_loop(0, rows_x, pack, 0, unroll=4)
        for direction in range(6):

            @pl.when(can_send(direction))
            def _():
                face(s, k, direction).start()

    def wait_faces(s, k):
        for direction in range(6):

            @pl.when(can_receive(direction))
            def _():
                face(s, k, direction).wait_recv()

    def wait_sent(s, k):
        for direction in range(6):

            @pl.when(can_send(direction))
            def _():
                face(s, k, direction).wait_send()

    zero = jnp.zeros((8, LANES), jnp.float32)

    def clear(direction):
        axis, side = AXES[direction // 2], direction % 2

        def clear_one(k, carry):
            if axis == "gx":
                plane = 0 if side else rows_x + 1
                for b in range(2):
                    for r in range(0, area, 8):
                        state[b, k, plane, rows_y + r : rows_y + r + 8, :] = zero
            elif axis == "gy":
                for s in range(SWEEPS):
                    for x in range(rows_x):
                        yrecv[s, side, k, x] = zero
            else:
                first = 0 if side else (blocks + 1) * rows_y
                for b in range(2):
                    for x in range(rows_x):
                        for r in range(0, rows_y, 8):
                            state[b, k, x + 1, first + r : first + r + 8, :] = zero
            return carry

        lax.fori_loop(0, K, clear_one, 0)

    for direction in range(6):

        @pl.when(jnp.logical_not(can_receive(direction)))
        def _():
            clear(direction)

    pl.semaphore_wait(barrier, peers)

    def first_sends(k, carry):
        for block in range(blocks):
            load(k, block).wait()
        send(0, k)
        return carry

    lax.fori_loop(0, K, first_sends, 0)

    def plane_sweep(s, k, x, store):
        b = s % 2
        for y in range(0, rows_y, 8):
            center = [
                state[b, k, x, n * rows_y + y : n * rows_y + y + 8, :] for n in range(blocks + 2)
            ]
            for n in range(1, blocks + 1):
                r = n * rows_y + y
                beside_x = state[b, k, x - 1, r : r + 8, :] + state[b, k, x + 1, r : r + 8, :]
                low = state[b, k, x, r - 1 : r + 7, :]
                high = state[b, k, x, r + 1 : r + 9, :]
                if y == 0:
                    edge = jnp.broadcast_to(yrecv[s, 1, k, x - 1, n - 1 : n, :], (8, LANES))
                    low = jnp.where(row == 0, edge, low)
                if y == rows_y - 8:
                    edge = jnp.broadcast_to(yrecv[s, 0, k, x - 1, n - 1 : n, :], (8, LANES))
                    high = jnp.where(row == 7, edge, high)
                left = pltpu.roll(jnp.where(lane == LANES - 1, center[n - 1], center[n]), 1, 1)
                right = pltpu.roll(jnp.where(lane == 0, center[n + 1], center[n]), LANES - 1, 1)
                value = keep * center[n] + weights[0] * beside_x
                value = value + weights[1] * (low + high)
                value = value + weights[2] * (left + right)
                store(n, y, value)

    for s in range(SWEEPS - 1):

        def one_vector(k, carry, s=s):
            wait_faces(s, k)
            if s > 0:
                wait_sent(s - 1, k)
            b = (s + 1) % 2

            def one_plane(x, carry):
                def store(n, y, value):
                    r = n * rows_y + y
                    state[b, k, x, r : r + 8, :] = value

                plane_sweep(s, k, x, store)
                return carry

            lax.fori_loop(1, rows_x + 1, one_plane, 0)
            send(s + 1, k)
            return carry

        lax.fori_loop(0, K, one_vector, 0)

    pick_row = lax.broadcasted_iota(jnp.int32, (2 * LANES, LANES), 0)
    pick_col = lax.broadcasted_iota(jnp.int32, (2 * LANES, LANES), 1)
    pick = jnp.where(pick_row // 2 == pick_col, 0.125, 0.0).astype(jnp.bfloat16)
    half_x, half_y = rows_x // 2, rows_y // 2
    s = SWEEPS - 1
    for k in range(K):
        wait_faces(s, k)

        def last_plane(x, sums):
            sums = list(sums)

            def store(n, y, value):
                window = (x - 1, slice(y, y + 8), slice((n - 1) * LANES, n * LANES))
                fields_ref[(k, *window)] = value
                for other in range(k):
                    sums[other] = sums[other] + value * fields_ref[(other, *window)]
                sums[k] = sums[k] + value * value

            plane_sweep(s, k, x, store)
            return tuple(sums)

        sums = lax.fori_loop(1, rows_x + 1, last_plane, (zero,) * (k + 1))
        for other in range(k + 1):
            fine_acc[k, other] = sums[other]

        def aggregate(i, carry):
            for n in range(blocks):
                columns = slice(n * LANES, (n + 1) * LANES)
                for y in range(0, rows_y, 8):
                    pairs[n, y : y + 8, :] = (
                        fields_ref[k, 2 * i, y : y + 8, columns]
                        + fields_ref[k, 2 * i + 1, y : y + 8, columns]
                    )
            for n in range(blocks):
                columns = slice(n * LANES, (n + 1) * LANES)
                quarter[i, :, columns] = (
                    pairs[n, pl.ds(0, half_y, stride=2), :]
                    + pairs[n, pl.ds(1, half_y, stride=2), :]
                )
            return carry

        lax.fori_loop(0, half_x, aggregate, 0)
        for n in range(0, blocks, 2):
            whole = quarter[:, :, n * LANES : (n + 2) * LANES]
            whole = whole.reshape(half_x * half_y, 2 * LANES)
            total = None
            for _ in range(3):
                part = whole.astype(jnp.bfloat16)
                whole = whole - part.astype(jnp.float32)
                product = jnp.dot(part, pick, preferred_element_type=jnp.float32)
                total = product if total is None else total + product
            columns = slice(n // 2 * LANES, (n // 2 + 1) * LANES)
            coarse_ref[k, :, :, columns] = total.reshape(half_x, half_y, LANES)

        def coarse_products(i, sums):
            sums = list(sums)
            for n in range(blocks // 2):
                columns = slice(n * LANES, (n + 1) * LANES)
                value = coarse_ref[k, i, :, columns]
                for other in range(k):
                    sums[other] = sums[other] + value * coarse_ref[other, i, :, columns]
                sums[k] = sums[k] + value * value
            return tuple(sums)

        sums = lax.fori_loop(0, half_x, coarse_products, (zero,) * (k + 1))
        for other in range(k + 1):
            coarse_acc[k, other] = sums[other]

    part = zero
    for which, acc in enumerate((fine_acc, coarse_acc)):
        for k in range(K):
            stacked = zero
            for other in range(K):
                tile = acc[max(k, other), min(k, other)]
                summed = jnp.sum(tile, axis=0, keepdims=True)
                stacked = jnp.where(row == other, summed, stacked)
            column = jnp.sum(stacked, axis=1, keepdims=True)
            part = jnp.where(lane == which * K + k, column, part)

    for number, (axis, slots) in enumerate((("gz", gather_z), ("gy", gather_y), ("gx", gather_x))):
        count = sizes[axis]
        me = position[axis]
        slots[me] = part

        def exchange(offset, axis=axis, slots=slots, me=me, count=count, number=number):
            return pltpu.make_async_remote_copy(
                src_ref=slots.at[me],
                dst_ref=slots.at[me],
                send_sem=gsend_sem.at[number, offset],
                recv_sem=grecv_sem.at[number, offset],
                device_id={axis: lax.rem(me + offset, count)},
                device_id_type=MESH,
            )

        def arrival(offset, axis=axis, slots=slots, me=me, count=count, number=number):
            source = lax.rem(me + count - offset, count)
            return pltpu.make_async_remote_copy(
                src_ref=slots.at[source],
                dst_ref=slots.at[source],
                send_sem=gsend_sem.at[number, offset],
                recv_sem=grecv_sem.at[number, offset],
                device_id={axis: source},
                device_id_type=MESH,
            )

        for offset in range(1, count):
            exchange(offset).start()
        for offset in range(1, count):
            arrival(offset).wait_recv()
        part = slots[0]
        for slot in range(1, count):
            part = part + slots[slot]
        for offset in range(1, count):
            exchange(offset).wait_send()
    gram_ref[...] = part

    def finish(k, carry):
        for s in range(SWEEPS - 2, SWEEPS):
            wait_sent(s, k)
        return carry

    lax.fori_loop(0, K, finish, 0)


def inverse_factor(gram, lane, row):
    work = jnp.where(lane < K, gram, 0.0) + jnp.where(lane == row + K, 1.0, 0.0)
    for j in range(K):
        pivot_row = jnp.broadcast_to(work[j : j + 1, :], work.shape)
        column = jnp.broadcast_to(work[:, j : j + 1], work.shape)
        pivot = jnp.broadcast_to(pivot_row[:, j : j + 1], work.shape)
        factor = jnp.where(row > j, column / pivot, 0.0)
        work = work - factor * pivot_row
    pivots = jnp.sum(jnp.where(lane == row, work, 0.0), axis=1, keepdims=True)
    scale = 1.0 / jnp.sqrt(pivots)
    return pltpu.roll(work * scale, LANES - K, 1)


def basis_kernel(
    cells,
    gram_ref,
    fields_ref,
    coarse_ref,
    basis_ref,
    coarse_basis_ref,
    stage,
    coarse_stage,
    table,
    out_sem,
    coarse_sem,
):
    rows_x, rows_y, blocks = (
        fields_ref.shape[1],
        fields_ref.shape[2],
        fields_ref.shape[3] // LANES,
    )
    lane = lax.broadcasted_iota(jnp.int32, (8, LANES), 1)
    row = lax.broadcasted_iota(jnp.int32, (8, LANES), 0)
    gram = gram_ref[...]
    fine = inverse_factor(gram / cells, lane, row)
    rest = inverse_factor(pltpu.roll(gram, LANES - K, 1) / (cells // 8), lane, row)
    for which, inverse in enumerate((fine, rest)):
        for other in range(K):
            table[which, other] = jnp.broadcast_to(inverse[:, other : other + 1], (8, LANES))

    def combine(which, windows, source, target):
        loaded = [[source(other, w) for w in windows] for other in range(K)]
        for k in range(K):
            totals = None
            for other in range(k + 1):
                weight = jnp.broadcast_to(table[which, other, k : k + 1, :], (8, LANES))
                products = [weight * value for value in loaded[other]]
                totals = (
                    products if totals is None else [t + p for t, p in zip(totals, products)]
                )
            for w, total in zip(windows, totals):
                target(k, w, total)

    def put(x):
        return pltpu.make_async_copy(stage.at[x], basis_ref.at[:, x], out_sem.at[x])

    def one_plane(x, carry):
        def source(k, w):
            return fields_ref[k, x, w[0] : w[0] + 8, w[1] * LANES : (w[1] + 1) * LANES]

        def target(k, w, value):
            stage[x, k, w[0] : w[0] + 8, w[1] * LANES : (w[1] + 1) * LANES] = value

        windows = [(y, n) for y in range(0, rows_y, 8) for n in range(blocks)]
        for first in range(0, len(windows), 4):
            combine(0, windows[first : first + 4], source, target)
        put(x).start()
        return carry

    lax.fori_loop(0, rows_x, one_plane, 0)

    def one_coarse(x, carry):
        def source(k, n):
            return coarse_ref[k, x, :, n * LANES : (n + 1) * LANES]

        def target(k, n, value):
            coarse_stage[k, x, :, n * LANES : (n + 1) * LANES] = value

        combine(1, list(range(blocks // 2)), source, target)
        return carry

    lax.fori_loop(0, rows_x // 2, one_coarse, 0)
    out = pltpu.make_async_copy(coarse_stage, coarse_basis_ref, coarse_sem)
    out.start()

    def drain(x, carry):
        put(x).wait()
        return carry

    lax.fori_loop(0, rows_x, drain, 0)
    out.wait()


def local(sizes, test_vectors, aniso):
    vectors, rows_x, rows_y, rows_z = test_vectors.shape
    blocks = rows_z // LANES
    half = (vectors, rows_x // 2, rows_y // 2, rows_z // 2)
    f32 = jnp.float32
    hbm = pl.BlockSpec(memory_space=pltpu.HBM)
    smem = pl.BlockSpec(memory_space=pltpu.SMEM)
    vmem = pl.BlockSpec(memory_space=pltpu.VMEM)
    longest = max(sizes.values())
    fields, coarse, gram = pl.pallas_call(
        functools.partial(sweep_kernel, sizes),
        out_shape=(
            pltpu.VMEM(test_vectors.shape, f32),
            pltpu.VMEM(half, f32),
            pltpu.VMEM((8, LANES), f32),
        ),
        in_specs=[smem, hbm],
        out_specs=(vmem, vmem, vmem),
        scratch_shapes=[
            pltpu.VMEM((2, vectors, rows_x + 2, (blocks + 2) * rows_y, LANES), f32),
            pltpu.VMEM((SWEEPS, 2, vectors, rows_x, blocks, LANES), f32),
            pltpu.VMEM((SWEEPS, 2, vectors, rows_x, blocks, LANES), f32),
            pltpu.VMEM((blocks, rows_y, LANES), f32),
            pltpu.VMEM((rows_x // 2, rows_y // 2, rows_z), f32),
            pltpu.VMEM((vectors, vectors, 8, LANES), f32),
            pltpu.VMEM((vectors, vectors, 8, LANES), f32),
            pltpu.VMEM((sizes["gz"], 8, LANES), f32),
            pltpu.VMEM((sizes["gy"], 8, LANES), f32),
            pltpu.VMEM((sizes["gx"], 8, LANES), f32),
            pltpu.SemaphoreType.DMA((vectors, blocks)),
            pltpu.SemaphoreType.DMA((6, SWEEPS, vectors)),
            pltpu.SemaphoreType.DMA((6, SWEEPS, vectors)),
            pltpu.SemaphoreType.DMA((3, longest)),
            pltpu.SemaphoreType.DMA((3, longest)),
        ],
        compiler_params=pltpu.CompilerParams(
            collective_id=0, has_side_effects=True, vmem_limit_bytes=44 * 1024 * 1024
        ),
        name="sweeps",
    )(aniso, test_vectors)
    cells = float(rows_x * rows_y * rows_z * sizes["gx"] * sizes["gy"] * sizes["gz"])
    return pl.pallas_call(
        functools.partial(basis_kernel, cells),
        out_shape=(
            jax.ShapeDtypeStruct(test_vectors.shape, f32),
            jax.ShapeDtypeStruct(half, f32),
        ),
        in_specs=[vmem, vmem, vmem],
        out_specs=(hbm, hbm),
        scratch_shapes=[
            pltpu.VMEM((rows_x, vectors, rows_y, rows_z), f32),
            pltpu.VMEM(half, f32),
            pltpu.VMEM((2, vectors, 8, LANES), f32),
            pltpu.SemaphoreType.DMA((rows_x,)),
            pltpu.SemaphoreType.DMA(()),
        ],
        compiler_params=pltpu.CompilerParams(vmem_limit_bytes=24 * 1024 * 1024),
        name="basis",
    )(gram, fields, coarse)


def solution(mesh):
    sizes = {axis: mesh.shape[axis] for axis in AXES}
    spec = P(None, "gx", "gy", "gz")
    return jax.shard_map(
        functools.partial(local, sizes),
        mesh=mesh,
        in_specs=(spec, P()),
        out_specs=(spec, spec),
        check_vma=False,
    )
```

```python
import functools

import jax
import jax.numpy as jnp
from jax import lax
from jax.experimental import pallas as pl
from jax.experimental.pallas import tpu as pltpu
from jax.sharding import PartitionSpec as P

MESH = pl.DeviceIdType.MESH
omega_weight = 2.0 / 3.0
K = 8
SWEEPS = 3
LANES = 128
AXES = ("gx", "gy", "gz")


def sweep_kernel(
    sizes,
    aniso_ref,
    in_ref,
    fields_ref,
    coarse_ref,
    gram_ref,
    even_state,
    odd_state,
    ysend,
    yrecv,
    pairs,
    fine_acc,
    coarse_acc,
    gather_z,
    gather_y,
    gather_x,
    load_sem,
    send_sem,
    recv_sem,
    gsend_sem,
    grecv_sem,
):
    rows_x, rows_y, blocks = (in_ref.shape[1], in_ref.shape[2], in_ref.shape[3] // LANES)
    area = blocks * rows_y
    states = (even_state, odd_state)
    position = {axis: lax.axis_index(axis) for axis in AXES}

    def load(k, block):
        return pltpu.make_async_copy(
            in_ref.at[k, :, :, pl.ds(block * LANES, LANES)],
            even_state.at[k, pl.ds(1, rows_x), pl.ds((block + 1) * rows_y, rows_y), :],
            load_sem.at[k, block],
        )

    def start_loads(k, carry):
        for block in range(blocks):
            load(k, block).start()
        return carry

    lax.fori_loop(0, K, start_loads, 0)

    barrier = pltpu.get_barrier_semaphore()
    peers = 0
    for axis in AXES:
        for offset in range(1, sizes[axis]):
            peer = lax.rem(position[axis] + offset, sizes[axis])
            pl.semaphore_signal(barrier, inc=1, device_id={axis: peer}, device_id_type=MESH)
            peers += 1

    def as_float(d, j):
        return jnp.full((8, LANES), aniso_ref[d, j], jnp.int32).astype(jnp.float32)

    coefficients = [as_float(d, 0) / as_float(d, 1) for d in range(3)]
    scaled = omega_weight / (2.0 * (coefficients[0] + coefficients[1] + coefficients[2]))
    weights = [scaled * c for c in coefficients]
    keep = 1.0 - omega_weight

    lane = lax.broadcasted_iota(jnp.int32, (8, LANES), 1)
    row = lax.broadcasted_iota(jnp.int32, (8, LANES), 0)

    def face(s, k, direction):
        state = states[s % 2]
        axis, side = AXES[direction // 2], direction % 2
        peer = position[axis] + (1 if side else -1)
        if axis == "gx":
            source = state.at[k, rows_x if side else 1, pl.ds(rows_y, area), :]
            target = state.at[k, 0 if side else rows_x + 1, pl.ds(rows_y, area), :]
        elif axis == "gy":
            source = ysend.at[s, side, k]
            target = yrecv.at[s, side, k]
        else:
            from_row = blocks * rows_y if side else rows_y
            to_row = 0 if side else (blocks + 1) * rows_y
            source = state.at[k, pl.ds(1, rows_x), pl.ds(from_row, rows_y), :]
            target = state.at[k, pl.ds(1, rows_x), pl.ds(to_row, rows_y), :]
        return pltpu.make_async_remote_copy(
            src_ref=source,
            dst_ref=target,
            send_sem=send_sem.at[direction, s, k],
            recv_sem=recv_sem.at[direction, s, k],
            device_id={axis: peer},
            device_id_type=MESH,
        )

    def can_send(direction):
        axis, side = AXES[direction // 2], direction % 2
        return position[axis] < sizes[axis] - 1 if side else position[axis] > 0

    def can_receive(direction):
        return can_send(direction ^ 1)

    def send(s, k):
        state = states[s % 2]

        def pack(x, carry):
            for side in range(2):
                first = rows_y + (rows_y - 1 if side else 0)
                ysend[s, side, k, x] = state[k, x + 1, pl.ds(first, blocks, stride=rows_y), :]
            return carry

        lax.fori_loop(0, rows_x, pack, 0, unroll=4)
        for direction in range(6):

            @pl.when(can_send(direction))
            def _():
                face(s, k, direction).start()

    def wait_faces(s, k):
        for direction in range(6):

            @pl.when(can_receive(direction))
            def _():
                face(s, k, direction).wait_recv()

    def wait_sent(s, k):
        for direction in range(6):

            @pl.when(can_send(direction))
            def _():
                face(s, k, direction).wait_send()

    zero = jnp.zeros((8, LANES), jnp.float32)

    def clear(direction):
        axis, side = AXES[direction // 2], direction % 2

        def clear_one(k, carry):
            if axis == "gx":
                plane = 0 if side else rows_x + 1
                for state in states:
                    for r in range(0, area, 8):
                        state[k, plane, rows_y + r : rows_y + r + 8, :] = zero
            elif axis == "gy":
                for s in range(SWEEPS):
                    for x in range(rows_x):
                        yrecv[s, side, k, x] = zero
            else:
                first = 0 if side else (blocks + 1) * rows_y
                for state in states:
                    for x in range(rows_x):
                        for r in range(0, rows_y, 8):
                            state[k, x + 1, first + r : first + r + 8, :] = zero
            return carry

        lax.fori_loop(0, K, clear_one, 0)

    for direction in range(6):

        @pl.when(jnp.logical_not(can_receive(direction)))
        def _():
            clear(direction)

    pl.semaphore_wait(barrier, peers)

    def first_sends(k, carry):
        for block in range(blocks):
            load(k, block).wait()
        send(0, k)
        return carry

    lax.fori_loop(0, K, first_sends, 0)

    def plane_sweep(s, k, x, store):
        state = states[s % 2]
        for y in range(0, rows_y, 8):
            center = [
                state[k, x, n * rows_y + y : n * rows_y + y + 8, :] for n in range(blocks + 2)
            ]
            for n in range(1, blocks + 1):
                r = n * rows_y + y
                beside_x = state[k, x - 1, r : r + 8, :] + state[k, x + 1, r : r + 8, :]
                low = state[k, x, r - 1 : r + 7, :]
                high = state[k, x, r + 1 : r + 9, :]
                if y == 0:
                    edge = jnp.broadcast_to(yrecv[s, 1, k, x - 1, n - 1 : n, :], (8, LANES))
                    low = jnp.where(row == 0, edge, low)
                if y == rows_y - 8:
                    edge = jnp.broadcast_to(yrecv[s, 0, k, x - 1, n - 1 : n, :], (8, LANES))
                    high = jnp.where(row == 7, edge, high)
                left = pltpu.roll(jnp.where(lane == LANES - 1, center[n - 1], center[n]), 1, 1)
                right = pltpu.roll(jnp.where(lane == 0, center[n + 1], center[n]), LANES - 1, 1)
                value = keep * center[n] + weights[0] * beside_x
                value = value + weights[1] * (low + high)
                value = value + weights[2] * (left + right)
                store(n, y, value)

    for s in range(SWEEPS - 1):

        def one_vector(k, carry, s=s):
            wait_faces(s, k)
            if s > 0:
                wait_sent(s - 1, k)
            after = states[(s + 1) % 2]

            def one_plane(x, carry):
                def store(n, y, value):
                    r = n * rows_y + y
                    after[k, x, r : r + 8, :] = value

                plane_sweep(s, k, x, store)
                return carry

            lax.fori_loop(1, rows_x + 1, one_plane, 0, unroll=4)
            send(s + 1, k)
            return carry

        lax.fori_loop(0, K, one_vector, 0)

    half_x, half_y = rows_x // 2, rows_y // 2
    compact = lax.rem(2 * lane, LANES)
    s = SWEEPS - 1
    for k in range(K):
        wait_faces(s, k)

        def last_planes(i, sums):
            fine, rest = list(sums[: k + 1]), list(sums[k + 1 :])
            found = {}
            for plane in range(2):

                def store(n, y, value, plane=plane):
                    window = (2 * i + plane, slice(y, y + 8), slice((n - 1) * LANES, n * LANES))
                    fields_ref[(k, *window)] = value
                    for other in range(k):
                        fine[other] = fine[other] + value * fields_ref[(other, *window)]
                    fine[k] = fine[k] + value * value
                    if plane:
                        pairs[n - 1, y : y + 8, :] = found.pop((n, y)) + value
                    else:
                        found[n, y] = value

                plane_sweep(s, k, 2 * i + 1 + plane, store)
            halves = []
            for n in range(blocks):
                value = (
                    pairs[n, pl.ds(0, half_y, stride=2), :]
                    + pairs[n, pl.ds(1, half_y, stride=2), :]
                )
                value = value + pltpu.roll(value, LANES - 1, 1)
                halves.append(jnp.take_along_axis(value, compact, axis=1))
            for n in range(blocks // 2):
                value = 0.125 * jnp.where(lane < LANES // 2, halves[2 * n], halves[2 * n + 1])
                window = (i, slice(None), slice(n * LANES, (n + 1) * LANES))
                coarse_ref[(k, *window)] = value
                for other in range(k):
                    rest[other] = rest[other] + value * coarse_ref[(other, *window)]
                rest[k] = rest[k] + value * value
            return (*fine, *rest)

        sums = lax.fori_loop(0, half_x, last_planes, (zero,) * (2 * k + 2))
        for other in range(k + 1):
            fine_acc[k, other] = sums[other]
            coarse_acc[k, other] = sums[k + 1 + other]

    part = zero
    for which, acc in enumerate((fine_acc, coarse_acc)):
        for k in range(K):
            stacked = zero
            for other in range(K):
                tile = acc[max(k, other), min(k, other)]
                summed = jnp.sum(tile, axis=0, keepdims=True)
                stacked = jnp.where(row == other, summed, stacked)
            column = jnp.sum(stacked, axis=1, keepdims=True)
            part = jnp.where(lane == which * K + k, column, part)

    for number, (axis, slots) in enumerate((("gz", gather_z), ("gy", gather_y), ("gx", gather_x))):
        count = sizes[axis]
        me = position[axis]
        slots[me] = part

        def exchange(offset, axis=axis, slots=slots, me=me, count=count, number=number):
            return pltpu.make_async_remote_copy(
                src_ref=slots.at[me],
                dst_ref=slots.at[me],
                send_sem=gsend_sem.at[number, offset],
                recv_sem=grecv_sem.at[number, offset],
                device_id={axis: lax.rem(me + offset, count)},
                device_id_type=MESH,
            )

        def arrival(offset, axis=axis, slots=slots, me=me, count=count, number=number):
            source = lax.rem(me + count - offset, count)
            return pltpu.make_async_remote_copy(
                src_ref=slots.at[source],
                dst_ref=slots.at[source],
                send_sem=gsend_sem.at[number, offset],
                recv_sem=grecv_sem.at[number, offset],
                device_id={axis: source},
                device_id_type=MESH,
            )

        for offset in range(1, count):
            exchange(offset).start()
        for offset in range(1, count):
            arrival(offset).wait_recv()
        part = slots[0]
        for slot in range(1, count):
            part = part + slots[slot]
        for offset in range(1, count):
            exchange(offset).wait_send()
    gram_ref[...] = part

    def finish(k, carry):
        for s in range(SWEEPS - 2, SWEEPS):
            wait_sent(s, k)
        return carry

    lax.fori_loop(0, K, finish, 0)


def inverse_factor(gram, lane, row):
    work = jnp.where(lane < K, gram, 0.0) + jnp.where(lane == row + K, 1.0, 0.0)
    for j in range(K):
        pivot_row = jnp.broadcast_to(work[j : j + 1, :], work.shape)
        column = jnp.broadcast_to(work[:, j : j + 1], work.shape)
        pivot = jnp.broadcast_to(pivot_row[:, j : j + 1], work.shape)
        factor = jnp.where(row > j, column / pivot, 0.0)
        work = work - factor * pivot_row
    pivots = jnp.sum(jnp.where(lane == row, work, 0.0), axis=1, keepdims=True)
    scale = 1.0 / jnp.sqrt(pivots)
    return pltpu.roll(work * scale, LANES - K, 1)


def basis_kernel(
    cells,
    gram_ref,
    fields_ref,
    coarse_ref,
    basis_ref,
    coarse_basis_ref,
    stage,
    coarse_stage,
    table,
    out_sem,
    coarse_sem,
):
    rows_x, rows_y, blocks = (
        fields_ref.shape[1],
        fields_ref.shape[2],
        fields_ref.shape[3] // LANES,
    )
    lane = lax.broadcasted_iota(jnp.int32, (8, LANES), 1)
    row = lax.broadcasted_iota(jnp.int32, (8, LANES), 0)
    gram = gram_ref[...]
    fine = inverse_factor(gram / cells, lane, row)
    rest = inverse_factor(pltpu.roll(gram, LANES - K, 1) / (cells // 8), lane, row)
    for which, inverse in enumerate((fine, rest)):
        for other in range(K):
            table[which, other] = jnp.broadcast_to(inverse[:, other : other + 1], (8, LANES))

    def combine(which, windows, source, target):
        loaded = [[source(other, w) for w in windows] for other in range(K)]
        for k in range(K):
            totals = None
            for other in range(k + 1):
                weight = jnp.broadcast_to(table[which, other, k : k + 1, :], (8, LANES))
                products = [weight * value for value in loaded[other]]
                totals = (
                    products if totals is None else [t + p for t, p in zip(totals, products)]
                )
            for w, total in zip(windows, totals):
                target(k, w, total)

    def put(x):
        return pltpu.make_async_copy(stage.at[x], basis_ref.at[:, x], out_sem.at[x])

    def one_plane(x, carry):
        def source(k, w):
            return fields_ref[k, x, w[0] : w[0] + 8, w[1] * LANES : (w[1] + 1) * LANES]

        def target(k, w, value):
            stage[x, k, w[0] : w[0] + 8, w[1] * LANES : (w[1] + 1) * LANES] = value

        windows = [(y, n) for y in range(0, rows_y, 8) for n in range(blocks)]
        for first in range(0, len(windows), 4):
            combine(0, windows[first : first + 4], source, target)
        put(x).start()
        return carry

    lax.fori_loop(0, rows_x, one_plane, 0)

    def one_coarse(x, carry):
        def source(k, n):
            return coarse_ref[k, x, :, n * LANES : (n + 1) * LANES]

        def target(k, n, value):
            coarse_stage[k, x, :, n * LANES : (n + 1) * LANES] = value

        combine(1, list(range(blocks // 2)), source, target)
        return carry

    lax.fori_loop(0, rows_x // 2, one_coarse, 0)
    out = pltpu.make_async_copy(coarse_stage, coarse_basis_ref, coarse_sem)
    out.start()

    def drain(x, carry):
        put(x).wait()
        return carry

    lax.fori_loop(0, rows_x, drain, 0)
    out.wait()


def local(sizes, test_vectors, aniso):
    vectors, rows_x, rows_y, rows_z = test_vectors.shape
    blocks = rows_z // LANES
    half = (vectors, rows_x // 2, rows_y // 2, rows_z // 2)
    f32 = jnp.float32
    hbm = pl.BlockSpec(memory_space=pltpu.HBM)
    smem = pl.BlockSpec(memory_space=pltpu.SMEM)
    vmem = pl.BlockSpec(memory_space=pltpu.VMEM)
    longest = max(sizes.values())
    fields, coarse, gram = pl.pallas_call(
        functools.partial(sweep_kernel, sizes),
        out_shape=(
            pltpu.VMEM(test_vectors.shape, f32),
            pltpu.VMEM(half, f32),
            pltpu.VMEM((8, LANES), f32),
        ),
        in_specs=[smem, hbm],
        out_specs=(vmem, vmem, vmem),
        scratch_shapes=[
            pltpu.VMEM((vectors, rows_x + 2, (blocks + 2) * rows_y, LANES), f32),
            pltpu.VMEM((vectors, rows_x + 2, (blocks + 2) * rows_y, LANES), f32),
            pltpu.VMEM((SWEEPS, 2, vectors, rows_x, blocks, LANES), f32),
            pltpu.VMEM((SWEEPS, 2, vectors, rows_x, blocks, LANES), f32),
            pltpu.VMEM((blocks, rows_y, LANES), f32),
            pltpu.VMEM((vectors, vectors, 8, LANES), f32),
            pltpu.VMEM((vectors, vectors, 8, LANES), f32),
            pltpu.VMEM((sizes["gz"], 8, LANES), f32),
            pltpu.VMEM((sizes["gy"], 8, LANES), f32),
            pltpu.VMEM((sizes["gx"], 8, LANES), f32),
            pltpu.SemaphoreType.DMA((vectors, blocks)),
            pltpu.SemaphoreType.DMA((6, SWEEPS, vectors)),
            pltpu.SemaphoreType.DMA((6, SWEEPS, vectors)),
            pltpu.SemaphoreType.DMA((3, longest)),
            pltpu.SemaphoreType.DMA((3, longest)),
        ],
        compiler_params=pltpu.CompilerParams(
            collective_id=0, has_side_effects=True, vmem_limit_bytes=44 * 1024 * 1024
        ),
        name="sweeps",
    )(aniso, test_vectors)
    cells = float(rows_x * rows_y * rows_z * sizes["gx"] * sizes["gy"] * sizes["gz"])
    return pl.pallas_call(
        functools.partial(basis_kernel, cells),
        out_shape=(
            jax.ShapeDtypeStruct(test_vectors.shape, f32),
            jax.ShapeDtypeStruct(half, f32),
        ),
        in_specs=[vmem, vmem, vmem],
        out_specs=(hbm, hbm),
        scratch_shapes=[
            pltpu.VMEM((rows_x, vectors, rows_y, rows_z), f32),
            pltpu.VMEM(half, f32),
            pltpu.VMEM((2, vectors, 8, LANES), f32),
            pltpu.SemaphoreType.DMA((rows_x,)),
            pltpu.SemaphoreType.DMA(()),
        ],
        compiler_params=pltpu.CompilerParams(vmem_limit_bytes=24 * 1024 * 1024),
        name="basis",
    )(gram, fields, coarse)


def solution(mesh):
    sizes = {axis: mesh.shape[axis] for axis in AXES}
    spec = P(None, "gx", "gy", "gz")
    return jax.shard_map(
        functools.partial(local, sizes),
        mesh=mesh,
        in_specs=(spec, P()),
        out_specs=(spec, spec),
        check_vma=False,
    )
```

```python
import functools
import itertools

import jax
import jax.numpy as jnp
from jax import lax
from jax.experimental import pallas as pl
from jax.experimental.pallas import tpu as pltpu
from jax.sharding import PartitionSpec as P

MESH = pl.DeviceIdType.MESH
omega_weight = 2.0 / 3.0
K = 8
SWEEPS = 3
LANES = 128
AXES = ("gx", "gy", "gz")
UNROLL = 8
UNROLL_LAST = 4
UNROLL_HALF = 2


NEAR = ("gz",)
FAR = ("gx", "gy")


def others(sizes, axes):
    return [o for o in itertools.product(*(range(sizes[a]) for a in axes)) if any(o)]


def shifted(sizes, position, axes, offsets):
    return {a: lax.rem(position[a] + o, sizes[a]) for a, o in zip(axes, offsets)}


def slot_of(sizes, where, axes):
    slot = 0
    for axis in axes:
        slot = slot * sizes[axis] + where[axis]
    return slot


def sweep_kernel(
    sizes,
    aniso_hbm,
    in_ref,
    fields_ref,
    coarse_ref,
    gram_ref,
    aniso_ref,
    even_state,
    odd_state,
    ysend,
    yrecv,
    pairs,
    sums_z,
    gather_near,
    gather_far,
    aniso_sem,
    load_sem,
    send_sem,
    recv_sem,
    near_send,
    near_recv,
    far_send,
    far_recv,
):
    rows_x, rows_y, blocks = (in_ref.shape[1], in_ref.shape[2], in_ref.shape[3] // LANES)
    area = blocks * rows_y
    states = (even_state, odd_state)
    position = {axis: lax.axis_index(axis) for axis in AXES}

    def load(k, block):
        return pltpu.make_async_copy(
            in_ref.at[k, :, :, pl.ds(block * LANES, LANES)],
            even_state.at[k, pl.ds(1, rows_x), pl.ds((block + 1) * rows_y, rows_y), :],
            load_sem.at[k, block],
        )

    def start_loads(k, carry):
        for block in range(blocks):
            load(k, block).start()
        return carry

    fetch = pltpu.make_async_copy(aniso_hbm, aniso_ref, aniso_sem)
    fetch.start()
    lax.fori_loop(0, K, start_loads, 0)

    barrier = pltpu.get_barrier_semaphore()
    peers = 0
    for axes in (NEAR, FAR):
        for offsets in others(sizes, axes):
            target = shifted(sizes, position, axes, offsets)
            pl.semaphore_signal(barrier, inc=1, device_id=target, device_id_type=MESH)
            peers += 1

    fetch.wait()

    def as_float(d, j):
        return jnp.full((8, LANES), aniso_ref[d, j], jnp.int32).astype(jnp.float32)

    coefficients = [as_float(d, 0) / as_float(d, 1) for d in range(3)]
    scaled = omega_weight / (2.0 * (coefficients[0] + coefficients[1] + coefficients[2]))
    weights = [scaled * c for c in coefficients]
    keep = 1.0 - omega_weight

    lane = lax.broadcasted_iota(jnp.int32, (8, LANES), 1)
    row = lax.broadcasted_iota(jnp.int32, (8, LANES), 0)

    def face(s, k, direction):
        state = states[s % 2]
        axis, side = AXES[direction // 2], direction % 2
        peer = position[axis] + (1 if side else -1)
        if axis == "gx":
            source = state.at[k, rows_x if side else 1, pl.ds(rows_y, area), :]
            target = state.at[k, 0 if side else rows_x + 1, pl.ds(rows_y, area), :]
        elif axis == "gy":
            source = ysend.at[s, side, k]
            target = yrecv.at[s, side, k]
        else:
            from_row = blocks * rows_y if side else rows_y
            to_row = 0 if side else (blocks + 1) * rows_y
            source = state.at[k, pl.ds(1, rows_x), pl.ds(from_row, rows_y), :]
            target = state.at[k, pl.ds(1, rows_x), pl.ds(to_row, rows_y), :]
        return pltpu.make_async_remote_copy(
            src_ref=source,
            dst_ref=target,
            send_sem=send_sem.at[direction, s, k],
            recv_sem=recv_sem.at[direction, s, k],
            device_id={axis: peer},
            device_id_type=MESH,
        )

    def can_send(direction):
        axis, side = AXES[direction // 2], direction % 2
        return position[axis] < sizes[axis] - 1 if side else position[axis] > 0

    def can_receive(direction):
        return can_send(direction ^ 1)

    def send(s, k):
        state = states[s % 2]

        def pack(x, carry):
            for side in range(2):
                first = rows_y + (rows_y - 1 if side else 0)
                ysend[s, side, k, x] = state[k, x + 1, pl.ds(first, blocks, stride=rows_y), :]
            return carry

        lax.fori_loop(0, rows_x, pack, 0, unroll=4)
        for direction in range(6):

            @pl.when(can_send(direction))
            def _():
                face(s, k, direction).start()

    def wait_faces(s, k):
        for direction in range(6):

            @pl.when(can_receive(direction))
            def _():
                face(s, k, direction).wait_recv()

    def wait_sent(s, k):
        for direction in range(6):

            @pl.when(can_send(direction))
            def _():
                face(s, k, direction).wait_send()

    zero = jnp.zeros((8, LANES), jnp.float32)

    def clear(direction):
        axis, side = AXES[direction // 2], direction % 2

        def clear_one(k, carry):
            if axis == "gx":
                plane = 0 if side else rows_x + 1
                for state in states:
                    for r in range(0, area, 8):
                        state[k, plane, rows_y + r : rows_y + r + 8, :] = zero
            elif axis == "gy":
                for s in range(SWEEPS):
                    for x in range(rows_x):
                        yrecv[s, side, k, x] = zero
            else:
                first = 0 if side else (blocks + 1) * rows_y
                for state in states:
                    for x in range(rows_x):
                        for r in range(0, rows_y, 8):
                            state[k, x + 1, first + r : first + r + 8, :] = zero
            return carry

        lax.fori_loop(0, K, clear_one, 0)

    for direction in range(6):

        @pl.when(jnp.logical_not(can_receive(direction)))
        def _():
            clear(direction)

    pl.semaphore_wait(barrier, peers)

    def first_sends(k, carry):
        for block in range(blocks):
            load(k, block).wait()
        send(0, k)
        return carry

    lax.fori_loop(0, K, first_sends, 0)

    def plane_sweep(s, k, x, store):
        state = states[s % 2]
        for y in range(0, rows_y, 8):
            center = [
                state[k, x, n * rows_y + y : n * rows_y + y + 8, :] for n in range(blocks + 2)
            ]
            for n in range(1, blocks + 1):
                r = n * rows_y + y
                beside_x = state[k, x - 1, r : r + 8, :] + state[k, x + 1, r : r + 8, :]
                low = state[k, x, r - 1 : r + 7, :]
                high = state[k, x, r + 1 : r + 9, :]
                if y == 0:
                    edge = jnp.broadcast_to(yrecv[s, 1, k, x - 1, n - 1 : n, :], (8, LANES))
                    low = jnp.where(row == 0, edge, low)
                if y == rows_y - 8:
                    edge = jnp.broadcast_to(yrecv[s, 0, k, x - 1, n - 1 : n, :], (8, LANES))
                    high = jnp.where(row == 7, edge, high)
                left = pltpu.roll(jnp.where(lane == LANES - 1, center[n - 1], center[n]), 1, 1)
                right = pltpu.roll(jnp.where(lane == 0, center[n + 1], center[n]), LANES - 1, 1)
                value = keep * center[n] + weights[0] * beside_x
                value = value + weights[1] * (low + high)
                value = value + weights[2] * (left + right)
                store(n, y, value)

    for s in range(SWEEPS - 1):

        def one_vector(k, carry, s=s):
            wait_faces(s, k)
            if s > 0:
                wait_sent(s - 1, k)
            after = states[(s + 1) % 2]

            def one_plane(x, carry):
                def store(n, y, value):
                    r = n * rows_y + y
                    after[k, x, r : r + 8, :] = value

                plane_sweep(s, k, x, store)
                return carry

            lax.fori_loop(1, rows_x + 1, one_plane, 0, unroll=UNROLL)
            send(s + 1, k)
            return carry

        lax.fori_loop(0, K, one_vector, 0)

    half_x, half_y = rows_x // 2, rows_y // 2
    even = lax.rem(lane, 2) == 0
    part = zero
    s = SWEEPS - 1

    def add_products(part, k, first, sums):
        stacked = zero
        for other in range(k + 1):
            summed = jnp.sum(sums[other], axis=0, keepdims=True)
            stacked = jnp.where(row == other, summed, stacked)
        column = jnp.broadcast_to(jnp.sum(stacked, axis=1, keepdims=True), (8, LANES))
        across = jnp.sum(jnp.where(lane == row + first, column, 0.0), axis=0, keepdims=True)
        part = jnp.where((lane == first + k) & (row <= k), column, part)
        inside = (row == k) & (lane >= first) & (lane < first + k)
        return jnp.where(inside, jnp.broadcast_to(across, (8, LANES)), part)

    for k in range(K):
        wait_faces(s, k)

        def last_plane(x, sums):
            fine = list(sums)

            def store(n, y, value):
                window = (x - 1, slice(y, y + 8), slice((n - 1) * LANES, n * LANES))
                fields_ref[(k, *window)] = value
                for other in range(k):
                    fine[other] = fine[other] + value * fields_ref[(other, *window)]
                fine[k] = fine[k] + value * value

            plane_sweep(s, k, x, store)
            return tuple(fine)

        fine = lax.fori_loop(1, rows_x + 1, last_plane, (zero,) * (k + 1), unroll=UNROLL_LAST)

        def aggregate(i, sums):
            rest = list(sums)
            for n in range(blocks):
                columns = slice(n * LANES, (n + 1) * LANES)
                for y in range(0, rows_y, 8):
                    pairs[n, y : y + 8, :] = (
                        fields_ref[k, 2 * i, y : y + 8, columns]
                        + fields_ref[k, 2 * i + 1, y : y + 8, columns]
                    )
            for n in range(blocks):
                value = (
                    pairs[n, pl.ds(0, half_y, stride=2), :]
                    + pairs[n, pl.ds(1, half_y, stride=2), :]
                )
                value = 0.125 * (value + pltpu.roll(value, LANES - 1, 1))
                value = jnp.where(even, value, 0.0)
                sums_z[k, i, n] = value
                for other in range(k):
                    rest[other] = rest[other] + value * sums_z[other, i, n]
                rest[k] = rest[k] + value * value
            return tuple(rest)

        rest = lax.fori_loop(0, half_x, aggregate, (zero,) * (k + 1), unroll=UNROLL_HALF)
        part = add_products(part, k, 0, fine)
        part = add_products(part, k, K, rest)

    def pack_lanes(k, carry):
        index = lax.rem(2 * lane, LANES)
        for i in range(half_x):
            for n in range(0, blocks, 2):
                low = jnp.take_along_axis(sums_z[k, i, n], index, axis=1)
                high = jnp.take_along_axis(sums_z[k, i, n + 1], index, axis=1)
                window = (i, slice(None), slice(n // 2 * LANES, (n // 2 + 1) * LANES))
                coarse_ref[(k, *window)] = jnp.where(lane < LANES // 2, low, high)
        return carry

    stages = (
        (NEAR, gather_near, near_send, near_recv),
        (FAR, gather_far, far_send, far_recv),
    )
    for stage, (axes, slots, sent, received) in enumerate(stages):
        me = slot_of(sizes, position, axes)
        group = others(sizes, axes)
        slots[me] = part

        def exchange(number, axes=axes, slots=slots, me=me, group=group, sent=sent, received=received):
            return pltpu.make_async_remote_copy(
                src_ref=slots.at[me],
                dst_ref=slots.at[me],
                send_sem=sent.at[number],
                recv_sem=received.at[number],
                device_id=shifted(sizes, position, axes, group[number]),
                device_id_type=MESH,
            )

        def arrival(number, axes=axes, slots=slots, group=group, sent=sent, received=received):
            back = tuple(sizes[a] - o for a, o in zip(axes, group[number]))
            where = shifted(sizes, position, axes, back)
            source = slot_of(sizes, where, axes)
            return pltpu.make_async_remote_copy(
                src_ref=slots.at[source],
                dst_ref=slots.at[source],
                send_sem=sent.at[number],
                recv_sem=received.at[number],
                device_id=where,
                device_id_type=MESH,
            )

        for number in range(len(group)):
            exchange(number).start()
        half = K // 2
        lax.fori_loop(stage * half, (stage + 1) * half, pack_lanes, 0)
        for number in range(len(group)):
            arrival(number).wait_recv()
        part = slots[0]
        for slot in range(1, len(group) + 1):
            part = part + slots[slot]
        for number in range(len(group)):
            exchange(number).wait_send()
    gram_ref[...] = part

    def finish(k, carry):
        for s in range(SWEEPS - 2, SWEEPS):
            wait_sent(s, k)
        return carry

    lax.fori_loop(0, K, finish, 0)


def inverse_factor(gram, lane, row):
    work = jnp.where(lane < K, gram, 0.0) + jnp.where(lane == row + K, 1.0, 0.0)
    for j in range(K):
        pivot_row = jnp.broadcast_to(work[j : j + 1, :], work.shape)
        column = jnp.broadcast_to(work[:, j : j + 1], work.shape)
        pivot = jnp.broadcast_to(pivot_row[:, j : j + 1], work.shape)
        factor = jnp.where(row > j, column / pivot, 0.0)
        work = work - factor * pivot_row
    pivots = jnp.sum(jnp.where(lane == row, work, 0.0), axis=1, keepdims=True)
    scale = 1.0 / jnp.sqrt(pivots)
    return pltpu.roll(work * scale, LANES - K, 1)


def basis_kernel(
    cells,
    gram_ref,
    fields_ref,
    coarse_ref,
    basis_ref,
    coarse_basis_ref,
    stage,
    coarse_stage,
    table,
    out_sem,
    coarse_sem,
):
    rows_x, rows_y, blocks = (
        fields_ref.shape[1],
        fields_ref.shape[2],
        fields_ref.shape[3] // LANES,
    )
    lane = lax.broadcasted_iota(jnp.int32, (8, LANES), 1)
    row = lax.broadcasted_iota(jnp.int32, (8, LANES), 0)
    gram = gram_ref[...]
    fine = inverse_factor(gram / cells, lane, row)
    rest = inverse_factor(pltpu.roll(gram, LANES - K, 1) / (cells // 8), lane, row)
    for which, inverse in enumerate((fine, rest)):
        for other in range(K):
            table[which, other] = jnp.broadcast_to(inverse[:, other : other + 1], (8, LANES))

    def combine(which, windows, source, target):
        loaded = [[source(other, w) for w in windows] for other in range(K)]
        for k in range(K):
            totals = None
            for other in range(k + 1):
                weight = jnp.broadcast_to(table[which, other, k : k + 1, :], (8, LANES))
                products = [weight * value for value in loaded[other]]
                totals = (
                    products if totals is None else [t + p for t, p in zip(totals, products)]
                )
            for w, total in zip(windows, totals):
                target(k, w, total)

    def put(x):
        return pltpu.make_async_copy(stage.at[x], basis_ref.at[:, x], out_sem.at[x])

    def one_plane(x, carry):
        def source(k, w):
            return fields_ref[k, x, w[0] : w[0] + 8, w[1] * LANES : (w[1] + 1) * LANES]

        def target(k, w, value):
            stage[x, k, w[0] : w[0] + 8, w[1] * LANES : (w[1] + 1) * LANES] = value

        windows = [(y, n) for y in range(0, rows_y, 8) for n in range(blocks)]
        for first in range(0, len(windows), 4):
            combine(0, windows[first : first + 4], source, target)
        put(x).start()
        return carry

    lax.fori_loop(0, rows_x, one_plane, 0)

    def one_coarse(x, carry):
        def source(k, n):
            return coarse_ref[k, x, :, n * LANES : (n + 1) * LANES]

        def target(k, n, value):
            coarse_stage[k, x, :, n * LANES : (n + 1) * LANES] = value

        combine(1, list(range(blocks // 2)), source, target)
        return carry

    lax.fori_loop(0, rows_x // 2, one_coarse, 0)
    out = pltpu.make_async_copy(coarse_stage, coarse_basis_ref, coarse_sem)
    out.start()

    def drain(x, carry):
        put(x).wait()
        return carry

    lax.fori_loop(0, rows_x, drain, 0)
    out.wait()


def local(sizes, test_vectors, aniso):
    vectors, rows_x, rows_y, rows_z = test_vectors.shape
    blocks = rows_z // LANES
    half = (vectors, rows_x // 2, rows_y // 2, rows_z // 2)
    f32 = jnp.float32
    hbm = pl.BlockSpec(memory_space=pltpu.HBM)
    vmem = pl.BlockSpec(memory_space=pltpu.VMEM)
    near, far = len(others(sizes, NEAR)), len(others(sizes, FAR))
    fields, coarse, gram = pl.pallas_call(
        functools.partial(sweep_kernel, sizes),
        out_shape=(
            pltpu.VMEM(test_vectors.shape, f32),
            pltpu.VMEM(half, f32),
            pltpu.VMEM((8, LANES), f32),
        ),
        in_specs=[hbm, hbm],
        out_specs=(vmem, vmem, vmem),
        scratch_shapes=[
            pltpu.SMEM(aniso.shape, jnp.int32),
            pltpu.VMEM((vectors, rows_x + 2, (blocks + 2) * rows_y, LANES), f32),
            pltpu.VMEM((vectors, rows_x + 2, (blocks + 2) * rows_y, LANES), f32),
            pltpu.VMEM((SWEEPS, 2, vectors, rows_x, blocks, LANES), f32),
            pltpu.VMEM((SWEEPS, 2, vectors, rows_x, blocks, LANES), f32),
            pltpu.VMEM((blocks, rows_y, LANES), f32),
            pltpu.VMEM((vectors, rows_x // 2, blocks, rows_y // 2, LANES), f32),
            pltpu.VMEM((near + 1, 8, LANES), f32),
            pltpu.VMEM((far + 1, 8, LANES), f32),
            pltpu.SemaphoreType.DMA(()),
            pltpu.SemaphoreType.DMA((vectors, blocks)),
            pltpu.SemaphoreType.DMA((6, SWEEPS, vectors)),
            pltpu.SemaphoreType.DMA((6, SWEEPS, vectors)),
            pltpu.SemaphoreType.DMA((near,)),
            pltpu.SemaphoreType.DMA((near,)),
            pltpu.SemaphoreType.DMA((far,)),
            pltpu.SemaphoreType.DMA((far,)),
        ],
        compiler_params=pltpu.CompilerParams(
            collective_id=0, has_side_effects=True, vmem_limit_bytes=44 * 1024 * 1024
        ),
        name="sweeps",
    )(aniso, test_vectors)
    cells = float(rows_x * rows_y * rows_z * sizes["gx"] * sizes["gy"] * sizes["gz"])
    return pl.pallas_call(
        functools.partial(basis_kernel, cells),
        out_shape=(
            jax.ShapeDtypeStruct(test_vectors.shape, f32),
            jax.ShapeDtypeStruct(half, f32),
        ),
        in_specs=[vmem, vmem, vmem],
        out_specs=(hbm, hbm),
        scratch_shapes=[
            pltpu.VMEM((rows_x, vectors, rows_y, rows_z), f32),
            pltpu.VMEM(half, f32),
            pltpu.VMEM((2, vectors, 8, LANES), f32),
            pltpu.SemaphoreType.DMA((rows_x,)),
            pltpu.SemaphoreType.DMA(()),
        ],
        compiler_params=pltpu.CompilerParams(vmem_limit_bytes=24 * 1024 * 1024),
        name="basis",
    )(gram, fields, coarse)


def solution(mesh):
    sizes = {axis: mesh.shape[axis] for axis in AXES}
    spec = P(None, "gx", "gy", "gz")
    return jax.shard_map(
        functools.partial(local, sizes),
        mesh=mesh,
        in_specs=(spec, P()),
        out_specs=(spec, spec),
        check_vma=False,
    )
```

```python
import functools
import itertools

import jax
import jax.numpy as jnp
from jax import lax
from jax.experimental import pallas as pl
from jax.experimental.pallas import tpu as pltpu
from jax.sharding import PartitionSpec as P

MESH = pl.DeviceIdType.MESH
omega_weight = 2.0 / 3.0
K = 8
SWEEPS = 3
LANES = 128
AXES = ("gx", "gy", "gz")
UNROLL = 8
GROUPS = (1,) * 8
UNROLL_LAST = 8
UNROLL_HALF = 4


NEAR = ("gz",)
FAR = ("gx", "gy")


def others(sizes, axes):
    return [o for o in itertools.product(*(range(sizes[a]) for a in axes)) if any(o)]


def shifted(sizes, position, axes, offsets):
    return {a: lax.rem(position[a] + o, sizes[a]) for a, o in zip(axes, offsets)}


def slot_of(sizes, where, axes):
    slot = 0
    for axis in axes:
        slot = slot * sizes[axis] + where[axis]
    return slot


def sweep_kernel(
    sizes,
    aniso_hbm,
    in_ref,
    fields_ref,
    coarse_ref,
    gram_ref,
    aniso_ref,
    even_state,
    odd_state,
    ysend,
    yrecv,
    pairs,
    sums_z,
    gather_near,
    gather_far,
    aniso_sem,
    load_sem,
    send_sem,
    recv_sem,
    near_send,
    near_recv,
    far_send,
    far_recv,
):
    rows_x, rows_y, blocks = (in_ref.shape[1], in_ref.shape[2], in_ref.shape[3] // LANES)
    area = blocks * rows_y
    states = (even_state, odd_state)
    position = {axis: lax.axis_index(axis) for axis in AXES}

    def load(k, block):
        return pltpu.make_async_copy(
            in_ref.at[k, :, :, pl.ds(block * LANES, LANES)],
            even_state.at[k, pl.ds(1, rows_x), pl.ds((block + 1) * rows_y, rows_y), :],
            load_sem.at[k, block],
        )

    def start_loads(k, carry):
        for block in range(blocks):
            load(k, block).start()
        return carry

    fetch = pltpu.make_async_copy(aniso_hbm, aniso_ref, aniso_sem)
    fetch.start()
    lax.fori_loop(0, K, start_loads, 0)

    barrier = pltpu.get_barrier_semaphore()
    peers = 0
    for axes in (NEAR, FAR):
        for offsets in others(sizes, axes):
            target = shifted(sizes, position, axes, offsets)
            pl.semaphore_signal(barrier, inc=1, device_id=target, device_id_type=MESH)
            peers += 1

    lane = lax.broadcasted_iota(jnp.int32, (8, LANES), 1)
    row = lax.broadcasted_iota(jnp.int32, (8, LANES), 0)

    starts = [sum(GROUPS[:g]) for g in range(len(GROUPS))]

    def face(s, g, direction):
        vectors = pl.ds(starts[g], GROUPS[g])
        state = states[s % 2]
        axis, side = AXES[direction // 2], direction % 2
        peer = position[axis] + (1 if side else -1)
        if axis == "gx":
            source = state.at[vectors, rows_x if side else 1, pl.ds(rows_y, area), :]
            target = state.at[vectors, 0 if side else rows_x + 1, pl.ds(rows_y, area), :]
        elif axis == "gy":
            source = ysend.at[s, side, vectors]
            target = yrecv.at[s, side, vectors]
        else:
            from_row = blocks * rows_y if side else rows_y
            to_row = 0 if side else (blocks + 1) * rows_y
            source = state.at[vectors, pl.ds(1, rows_x), pl.ds(from_row, rows_y), :]
            target = state.at[vectors, pl.ds(1, rows_x), pl.ds(to_row, rows_y), :]
        return pltpu.make_async_remote_copy(
            src_ref=source,
            dst_ref=target,
            send_sem=send_sem.at[direction, s, g],
            recv_sem=recv_sem.at[direction, s, g],
            device_id={axis: peer},
            device_id_type=MESH,
        )

    def can_send(direction):
        axis, side = AXES[direction // 2], direction % 2
        return position[axis] < sizes[axis] - 1 if side else position[axis] > 0

    def can_receive(direction):
        return can_send(direction ^ 1)

    def pack(s, k):
        state = states[s % 2]

        def pack_plane(x, carry):
            for side in range(2):
                first = rows_y + (rows_y - 1 if side else 0)
                ysend[s, side, k, x] = state[k, x + 1, pl.ds(first, blocks, stride=rows_y), :]
            return carry

        lax.fori_loop(0, rows_x, pack_plane, 0, unroll=4)

    def send(s, g):
        for direction in range(6):

            @pl.when(can_send(direction))
            def _():
                face(s, g, direction).start()

    def wait_faces(s, g):
        for direction in range(6):

            @pl.when(can_receive(direction))
            def _():
                face(s, g, direction).wait_recv()

    def wait_sent(s, g):
        for direction in range(6):

            @pl.when(can_send(direction))
            def _():
                face(s, g, direction).wait_send()

    zero = jnp.zeros((8, LANES), jnp.float32)

    def clear(direction):
        axis, side = AXES[direction // 2], direction % 2

        def clear_one(k, carry):
            if axis == "gx":
                plane = 0 if side else rows_x + 1
                for state in states:
                    for r in range(0, area, 8):
                        state[k, plane, rows_y + r : rows_y + r + 8, :] = zero
            elif axis == "gy":
                for s in range(SWEEPS):
                    for x in range(rows_x):
                        yrecv[s, side, k, x] = zero
            else:
                first = 0 if side else (blocks + 1) * rows_y
                for state in states:
                    for x in range(rows_x):
                        for r in range(0, rows_y, 8):
                            state[k, x + 1, first + r : first + r + 8, :] = zero
            return carry

        lax.fori_loop(0, K, clear_one, 0)

    pl.semaphore_wait(barrier, peers)

    def loaded(k, carry):
        for block in range(blocks):
            load(k, block).wait()
        pack(0, k)
        return carry

    for g, size in enumerate(GROUPS):
        lax.fori_loop(starts[g], starts[g] + size, loaded, 0)
        send(0, g)

    for direction in range(6):

        @pl.when(jnp.logical_not(can_receive(direction)))
        def _():
            clear(direction)

    fetch.wait()

    def as_float(d, j):
        return jnp.full((8, LANES), aniso_ref[d, j], jnp.int32).astype(jnp.float32)

    coefficients = [as_float(d, 0) / as_float(d, 1) for d in range(3)]
    scaled = omega_weight / (2.0 * (coefficients[0] + coefficients[1] + coefficients[2]))
    weights = [scaled * c for c in coefficients]
    keep = 1.0 - omega_weight

    def plane_sweep(s, k, x, store):
        state = states[s % 2]
        for y in range(0, rows_y, 8):
            center = [
                state[k, x, n * rows_y + y : n * rows_y + y + 8, :] for n in range(blocks + 2)
            ]
            for n in range(1, blocks + 1):
                r = n * rows_y + y
                beside_x = state[k, x - 1, r : r + 8, :] + state[k, x + 1, r : r + 8, :]
                low = state[k, x, r - 1 : r + 7, :]
                high = state[k, x, r + 1 : r + 9, :]
                if y == 0:
                    edge = jnp.broadcast_to(yrecv[s, 1, k, x - 1, n - 1 : n, :], (8, LANES))
                    low = jnp.where(row == 0, edge, low)
                if y == rows_y - 8:
                    edge = jnp.broadcast_to(yrecv[s, 0, k, x - 1, n - 1 : n, :], (8, LANES))
                    high = jnp.where(row == 7, edge, high)
                left = pltpu.roll(jnp.where(lane == LANES - 1, center[n - 1], center[n]), 1, 1)
                right = pltpu.roll(jnp.where(lane == 0, center[n + 1], center[n]), LANES - 1, 1)
                value = keep * center[n] + weights[0] * beside_x
                value = value + weights[1] * (low + high)
                value = value + weights[2] * (left + right)
                store(n, y, value)

    for s in range(SWEEPS - 1):
        for g, size in enumerate(GROUPS):
            wait_faces(s, g)
            if s > 0:
                wait_sent(s - 1, g)
            after = states[(s + 1) % 2]

            def one_vector(k, carry, s=s, after=after):
                def one_plane(x, carry):
                    def store(n, y, value):
                        r = n * rows_y + y
                        after[k, x, r : r + 8, :] = value

                    plane_sweep(s, k, x, store)
                    return carry

                lax.fori_loop(1, rows_x + 1, one_plane, 0, unroll=UNROLL)
                pack(s + 1, k)
                return carry

            lax.fori_loop(starts[g], starts[g] + size, one_vector, 0)
            send(s + 1, g)

    half_x, half_y = rows_x // 2, rows_y // 2
    even = lax.rem(lane, 2) == 0
    part = zero
    s = SWEEPS - 1

    def add_products(part, k, first, sums):
        stacked = zero
        for other in range(k + 1):
            summed = jnp.sum(sums[other], axis=0, keepdims=True)
            stacked = jnp.where(row == other, summed, stacked)
        column = jnp.broadcast_to(jnp.sum(stacked, axis=1, keepdims=True), (8, LANES))
        across = jnp.sum(jnp.where(lane == row + first, column, 0.0), axis=0, keepdims=True)
        part = jnp.where((lane == first + k) & (row <= k), column, part)
        inside = (row == k) & (lane >= first) & (lane < first + k)
        return jnp.where(inside, jnp.broadcast_to(across, (8, LANES)), part)

    for k in range(K):
        if k in starts:
            wait_faces(s, starts.index(k))

        def last_plane(x, sums):
            fine = list(sums)

            def store(n, y, value):
                window = (x - 1, slice(y, y + 8), slice((n - 1) * LANES, n * LANES))
                fields_ref[(k, *window)] = value
                for other in range(k):
                    fine[other] = fine[other] + value * fields_ref[(other, *window)]
                fine[k] = fine[k] + value * value

            plane_sweep(s, k, x, store)
            return tuple(fine)

        fine = lax.fori_loop(1, rows_x + 1, last_plane, (zero,) * (k + 1), unroll=UNROLL_LAST)

        part = add_products(part, k, 0, fine)

        def aggregate(i, sums):
            rest = list(sums)
            for n in range(blocks):
                columns = slice(n * LANES, (n + 1) * LANES)
                for y in range(0, rows_y, 8):
                    pairs[n, y : y + 8, :] = (
                        fields_ref[k, 2 * i, y : y + 8, columns]
                        + fields_ref[k, 2 * i + 1, y : y + 8, columns]
                    )
            for n in range(blocks):
                value = (
                    pairs[n, pl.ds(0, half_y, stride=2), :]
                    + pairs[n, pl.ds(1, half_y, stride=2), :]
                )
                value = 0.125 * (value + pltpu.roll(value, LANES - 1, 1))
                value = jnp.where(even, value, 0.0)
                sums_z[k, i, n] = value
                for other in range(k):
                    rest[other] = rest[other] + value * sums_z[other, i, n]
                rest[k] = rest[k] + value * value
            return tuple(rest)

        rest = lax.fori_loop(0, half_x, aggregate, (zero,) * (k + 1), unroll=UNROLL_HALF)
        part = add_products(part, k, K, rest)

    def pack_lanes(k, carry):
        index = lax.rem(2 * lane, LANES)
        for i in range(half_x):
            for n in range(0, blocks, 2):
                low = jnp.take_along_axis(sums_z[k, i, n], index, axis=1)
                high = jnp.take_along_axis(sums_z[k, i, n + 1], index, axis=1)
                window = (i, slice(None), slice(n // 2 * LANES, (n // 2 + 1) * LANES))
                coarse_ref[(k, *window)] = jnp.where(lane < LANES // 2, low, high)
        return carry

    stages = (
        (NEAR, gather_near, near_send, near_recv),
        (FAR, gather_far, far_send, far_recv),
    )
    for stage, (axes, slots, sent, received) in enumerate(stages):
        me = slot_of(sizes, position, axes)
        group = others(sizes, axes)
        slots[me] = part

        def exchange(number, axes=axes, slots=slots, me=me, group=group, sent=sent, received=received):
            return pltpu.make_async_remote_copy(
                src_ref=slots.at[me],
                dst_ref=slots.at[me],
                send_sem=sent.at[number],
                recv_sem=received.at[number],
                device_id=shifted(sizes, position, axes, group[number]),
                device_id_type=MESH,
            )

        def arrival(number, axes=axes, slots=slots, group=group, sent=sent, received=received):
            back = tuple(sizes[a] - o for a, o in zip(axes, group[number]))
            where = shifted(sizes, position, axes, back)
            source = slot_of(sizes, where, axes)
            return pltpu.make_async_remote_copy(
                src_ref=slots.at[source],
                dst_ref=slots.at[source],
                send_sem=sent.at[number],
                recv_sem=received.at[number],
                device_id=where,
                device_id_type=MESH,
            )

        for number in range(len(group)):
            exchange(number).start()
        half = K // 2
        lax.fori_loop(stage * half, (stage + 1) * half, pack_lanes, 0)
        for number in range(len(group)):
            arrival(number).wait_recv()
        part = slots[0]
        for slot in range(1, len(group) + 1):
            part = part + slots[slot]
        for number in range(len(group)):
            exchange(number).wait_send()
    gram_ref[...] = part

    for s in range(SWEEPS - 2, SWEEPS):
        for g in range(len(GROUPS)):
            wait_sent(s, g)


def inverse_factor(entry):
    left = {(k, j): entry(k, j) for k in range(K) for j in range(k + 1)}
    factor, inverse, scale = {}, {}, []
    for j in range(K):
        scale.append(lax.rsqrt(left[j, j]))
        reciprocal = 1.0 / left[j, j]
        for k in range(j + 1, K):
            factor[k, j] = left[k, j] * reciprocal
        for k in range(j + 1, K):
            for other in range(j + 1, k + 1):
                left[k, other] = left[k, other] - factor[k, j] * left[other, j]
    for k in range(K):
        for j in range(k):
            total = factor[k, j]
            for other in range(j + 1, k):
                total = total + factor[k, other] * inverse[other, j]
            inverse[k, j] = -total
    result = {(k, j): scale[k] * inverse[k, j] for k in range(K) for j in range(k)}
    result.update({(k, k): scale[k] for k in range(K)})
    return result


def basis_kernel(
    cells,
    gram_ref,
    fields_ref,
    coarse_ref,
    basis_ref,
    coarse_basis_ref,
    stage,
    coarse_stage,
    columns,
    table,
    out_sem,
    coarse_sem,
):
    rows_x, rows_y, blocks = (
        fields_ref.shape[1],
        fields_ref.shape[2],
        fields_ref.shape[3] // LANES,
    )
    gram = gram_ref[...]
    for which, count in enumerate((cells, cells // 8)):
        mean = gram / count
        for j in range(K):
            c = which * K + j
            columns[c] = jnp.broadcast_to(mean[:, c : c + 1], (8, LANES))
    for which in range(2):

        def entry(k, j, which=which):
            return jnp.broadcast_to(columns[which * K + j, k : k + 1, :], (8, LANES))

        for (k, j), value in inverse_factor(entry).items():
            table[which, k * (k + 1) // 2 + j] = value

    def combine(which, windows, source, target):
        loaded = [[source(other, w) for w in windows] for other in range(K)]
        for k in range(K):
            totals = None
            for other in range(k + 1):
                weight = table[which, k * (k + 1) // 2 + other]
                products = [weight * value for value in loaded[other]]
                totals = (
                    products if totals is None else [t + p for t, p in zip(totals, products)]
                )
            for w, total in zip(windows, totals):
                target(k, w, total)

    def put(x):
        return pltpu.make_async_copy(stage.at[x], basis_ref.at[:, x], out_sem.at[x])

    def one_plane(x, carry):
        def source(k, w):
            return fields_ref[k, x, w[0] : w[0] + 8, w[1] * LANES : (w[1] + 1) * LANES]

        def target(k, w, value):
            stage[x, k, w[0] : w[0] + 8, w[1] * LANES : (w[1] + 1) * LANES] = value

        windows = [(y, n) for y in range(0, rows_y, 8) for n in range(blocks)]
        for first in range(0, len(windows), 4):
            combine(0, windows[first : first + 4], source, target)
        put(x).start()
        return carry

    def one_coarse(x, carry):
        def source(k, n):
            return coarse_ref[k, x, :, n * LANES : (n + 1) * LANES]

        def target(k, n, value):
            coarse_stage[k, x, :, n * LANES : (n + 1) * LANES] = value

        combine(1, list(range(blocks // 2)), source, target)
        return carry

    lax.fori_loop(0, rows_x // 2, one_plane, 0)
    lax.fori_loop(0, rows_x // 2, one_coarse, 0)
    out = pltpu.make_async_copy(coarse_stage, coarse_basis_ref, coarse_sem)
    out.start()
    lax.fori_loop(rows_x // 2, rows_x, one_plane, 0)

    def drain(x, carry):
        put(x).wait()
        return carry

    lax.fori_loop(0, rows_x, drain, 0)
    out.wait()


def local(sizes, test_vectors, aniso):
    vectors, rows_x, rows_y, rows_z = test_vectors.shape
    blocks = rows_z // LANES
    half = (vectors, rows_x // 2, rows_y // 2, rows_z // 2)
    f32 = jnp.float32
    hbm = pl.BlockSpec(memory_space=pltpu.HBM)
    vmem = pl.BlockSpec(memory_space=pltpu.VMEM)
    near, far = len(others(sizes, NEAR)), len(others(sizes, FAR))
    fields, coarse, gram = pl.pallas_call(
        functools.partial(sweep_kernel, sizes),
        out_shape=(
            pltpu.VMEM(test_vectors.shape, f32),
            pltpu.VMEM(half, f32),
            pltpu.VMEM((8, LANES), f32),
        ),
        in_specs=[hbm, hbm],
        out_specs=(vmem, vmem, vmem),
        scratch_shapes=[
            pltpu.SMEM(aniso.shape, jnp.int32),
            pltpu.VMEM((vectors, rows_x + 2, (blocks + 2) * rows_y, LANES), f32),
            pltpu.VMEM((vectors, rows_x + 2, (blocks + 2) * rows_y, LANES), f32),
            pltpu.VMEM((SWEEPS, 2, vectors, rows_x, blocks, LANES), f32),
            pltpu.VMEM((SWEEPS, 2, vectors, rows_x, blocks, LANES), f32),
            pltpu.VMEM((blocks, rows_y, LANES), f32),
            pltpu.VMEM((vectors, rows_x // 2, blocks, rows_y // 2, LANES), f32),
            pltpu.VMEM((near + 1, 8, LANES), f32),
            pltpu.VMEM((far + 1, 8, LANES), f32),
            pltpu.SemaphoreType.DMA(()),
            pltpu.SemaphoreType.DMA((vectors, blocks)),
            pltpu.SemaphoreType.DMA((6, SWEEPS, len(GROUPS))),
            pltpu.SemaphoreType.DMA((6, SWEEPS, len(GROUPS))),
            pltpu.SemaphoreType.DMA((near,)),
            pltpu.SemaphoreType.DMA((near,)),
            pltpu.SemaphoreType.DMA((far,)),
            pltpu.SemaphoreType.DMA((far,)),
        ],
        compiler_params=pltpu.CompilerParams(
            collective_id=0, has_side_effects=True, vmem_limit_bytes=44 * 1024 * 1024
        ),
        name="sweeps",
    )(aniso, test_vectors)
    cells = float(rows_x * rows_y * rows_z * sizes["gx"] * sizes["gy"] * sizes["gz"])
    return pl.pallas_call(
        functools.partial(basis_kernel, cells),
        out_shape=(
            jax.ShapeDtypeStruct(test_vectors.shape, f32),
            jax.ShapeDtypeStruct(half, f32),
        ),
        in_specs=[vmem, vmem, vmem],
        out_specs=(hbm, hbm),
        scratch_shapes=[
            pltpu.VMEM((rows_x, vectors, rows_y, rows_z), f32),
            pltpu.VMEM(half, f32),
            pltpu.VMEM((2 * vectors, 8, LANES), f32),
            pltpu.VMEM((2, vectors * (vectors + 1) // 2, 8, LANES), f32),
            pltpu.SemaphoreType.DMA((rows_x,)),
            pltpu.SemaphoreType.DMA(()),
        ],
        compiler_params=pltpu.CompilerParams(vmem_limit_bytes=24 * 1024 * 1024),
        name="basis",
    )(gram, fields, coarse)


def solution(mesh):
    sizes = {axis: mesh.shape[axis] for axis in AXES}
    spec = P(None, "gx", "gy", "gz")
    return jax.shard_map(
        functools.partial(local, sizes),
        mesh=mesh,
        in_specs=(spec, P()),
        out_specs=(spec, spec),
        check_vma=False,
    )
```

```python
import functools
import itertools

import jax
import jax.numpy as jnp
from jax import lax
from jax.experimental import pallas as pl
from jax.experimental.pallas import tpu as pltpu
from jax.sharding import PartitionSpec as P

MESH = pl.DeviceIdType.MESH
omega_weight = 2.0 / 3.0
K = 8
SWEEPS = 3
LANES = 128
AXES = ("gx", "gy", "gz")
UNROLL = 8
GROUPS = (1,) * 8
UNROLL_LAST = 8
UNROLL_HALF = 4


NEAR = ("gz",)
FAR = ("gx", "gy")
ROUNDS = (
    (("gz", 1), ("gx", 1)),
    (("gz", 2), ("gx", 2)),
    (("gz", 4), ("gy", 1)),
    (("gy", 1),),
    (("gy", 2),),
)


def others(sizes, axes):
    return [o for o in itertools.product(*(range(sizes[a]) for a in axes)) if any(o)]


def shifted(sizes, position, axes, offsets):
    return {a: lax.rem(position[a] + o, sizes[a]) for a, o in zip(axes, offsets)}


def slot_of(sizes, where, axes):
    slot = 0
    for axis in axes:
        slot = slot * sizes[axis] + where[axis]
    return slot


def sweep_kernel(
    sizes,
    aniso_hbm,
    in_ref,
    fields_ref,
    coarse_ref,
    gram_ref,
    aniso_ref,
    even_state,
    odd_state,
    ysend,
    yrecv,
    pairs,
    sums_z,
    gather_near,
    gather_far,
    aniso_sem,
    load_sem,
    send_sem,
    recv_sem,
    near_send,
    near_recv,
    far_send,
    far_recv,
    rounds,
):
    rows_x, rows_y, blocks = (in_ref.shape[1], in_ref.shape[2], in_ref.shape[3] // LANES)
    area = blocks * rows_y
    states = (even_state, odd_state)
    position = {axis: lax.axis_index(axis) for axis in AXES}

    def load(k, block):
        return pltpu.make_async_copy(
            in_ref.at[k, :, :, pl.ds(block * LANES, LANES)],
            even_state.at[k, pl.ds(1, rows_x), pl.ds((block + 1) * rows_y, rows_y), :],
            load_sem.at[k, block],
        )

    def start_loads(k, carry):
        for block in range(blocks):
            load(k, block).start()
        return carry

    fetch = pltpu.make_async_copy(aniso_hbm, aniso_ref, aniso_sem)
    fetch.start()
    lax.fori_loop(0, K, start_loads, 0)

    def greet(semaphore, axis, distance):
        heard = 0
        for step in (-distance, distance):
            there = position[axis] >= distance if step < 0 else position[axis] < sizes[axis] - distance

            @pl.when(there)
            def _():
                pl.semaphore_signal(
                    semaphore,
                    inc=1,
                    device_id={axis: position[axis] + step},
                    device_id_type=MESH,
                )

            heard = heard + there.astype(jnp.int32)
        return heard

    barrier = pltpu.get_barrier_semaphore()
    peers = sum(greet(barrier, axis, 1) for axis in AXES)

    def hear(number):
        heard = sum(greet(rounds.at[number], axis, d) for axis, d in ROUNDS[number])
        pl.semaphore_wait(rounds.at[number], heard)

    lane = lax.broadcasted_iota(jnp.int32, (8, LANES), 1)
    row = lax.broadcasted_iota(jnp.int32, (8, LANES), 0)

    starts = [sum(GROUPS[:g]) for g in range(len(GROUPS))]

    def face(s, g, direction):
        vectors = pl.ds(starts[g], GROUPS[g])
        state = states[s % 2]
        axis, side = AXES[direction // 2], direction % 2
        peer = position[axis] + (1 if side else -1)
        if axis == "gx":
            source = state.at[vectors, rows_x if side else 1, pl.ds(rows_y, area), :]
            target = state.at[vectors, 0 if side else rows_x + 1, pl.ds(rows_y, area), :]
        elif axis == "gy":
            source = ysend.at[s, side, vectors]
            target = yrecv.at[s, side, vectors]
        else:
            from_row = blocks * rows_y if side else rows_y
            to_row = 0 if side else (blocks + 1) * rows_y
            source = state.at[vectors, pl.ds(1, rows_x), pl.ds(from_row, rows_y), :]
            target = state.at[vectors, pl.ds(1, rows_x), pl.ds(to_row, rows_y), :]
        return pltpu.make_async_remote_copy(
            src_ref=source,
            dst_ref=target,
            send_sem=send_sem.at[direction, s, g],
            recv_sem=recv_sem.at[direction, s, g],
            device_id={axis: peer},
            device_id_type=MESH,
        )

    def can_send(direction):
        axis, side = AXES[direction // 2], direction % 2
        return position[axis] < sizes[axis] - 1 if side else position[axis] > 0

    def can_receive(direction):
        return can_send(direction ^ 1)

    def pack(s, k):
        state = states[s % 2]

        def pack_plane(x, carry):
            for side in range(2):
                first = rows_y + (rows_y - 1 if side else 0)
                ysend[s, side, k, x] = state[k, x + 1, pl.ds(first, blocks, stride=rows_y), :]
            return carry

        lax.fori_loop(0, rows_x, pack_plane, 0, unroll=4)

    def send(s, g):
        for direction in range(6):

            @pl.when(can_send(direction))
            def _():
                face(s, g, direction).start()

    def wait_faces(s, g):
        for direction in range(6):

            @pl.when(can_receive(direction))
            def _():
                face(s, g, direction).wait_recv()

    def wait_sent(s, g):
        for direction in range(6):

            @pl.when(can_send(direction))
            def _():
                face(s, g, direction).wait_send()

    zero = jnp.zeros((8, LANES), jnp.float32)

    def clear(direction):
        axis, side = AXES[direction // 2], direction % 2

        def clear_one(k, carry):
            if axis == "gx":
                plane = 0 if side else rows_x + 1
                for state in states:
                    for r in range(0, area, 8):
                        state[k, plane, rows_y + r : rows_y + r + 8, :] = zero
            elif axis == "gy":
                for s in range(SWEEPS):
                    for x in range(rows_x):
                        yrecv[s, side, k, x] = zero
            else:
                first = 0 if side else (blocks + 1) * rows_y
                for state in states:
                    for x in range(rows_x):
                        for r in range(0, rows_y, 8):
                            state[k, x + 1, first + r : first + r + 8, :] = zero
            return carry

        lax.fori_loop(0, K, clear_one, 0)

    pl.semaphore_wait(barrier, peers)

    def loaded(k, carry):
        for block in range(blocks):
            load(k, block).wait()
        pack(0, k)
        return carry

    for g, size in enumerate(GROUPS):
        lax.fori_loop(starts[g], starts[g] + size, loaded, 0)
        send(0, g)

    for direction in range(6):

        @pl.when(jnp.logical_not(can_receive(direction)))
        def _():
            clear(direction)

    fetch.wait()

    def as_float(d, j):
        return jnp.full((8, LANES), aniso_ref[j, d], jnp.int32).astype(jnp.float32)

    coefficients = [as_float(d, 0) / as_float(d, 1) for d in range(3)]
    scaled = omega_weight / (2.0 * (coefficients[0] + coefficients[1] + coefficients[2]))
    weights = [scaled * c for c in coefficients]
    keep = 1.0 - omega_weight

    def plane_sweep(s, k, x, store):
        state = states[s % 2]
        for y in range(0, rows_y, 8):
            center = [
                state[k, x, n * rows_y + y : n * rows_y + y + 8, :] for n in range(blocks + 2)
            ]
            for n in range(1, blocks + 1):
                r = n * rows_y + y
                beside_x = state[k, x - 1, r : r + 8, :] + state[k, x + 1, r : r + 8, :]
                low = state[k, x, r - 1 : r + 7, :]
                high = state[k, x, r + 1 : r + 9, :]
                if y == 0:
                    edge = jnp.broadcast_to(yrecv[s, 1, k, x - 1, n - 1 : n, :], (8, LANES))
                    low = jnp.where(row == 0, edge, low)
                if y == rows_y - 8:
                    edge = jnp.broadcast_to(yrecv[s, 0, k, x - 1, n - 1 : n, :], (8, LANES))
                    high = jnp.where(row == 7, edge, high)
                left = pltpu.roll(jnp.where(lane == LANES - 1, center[n - 1], center[n]), 1, 1)
                right = pltpu.roll(jnp.where(lane == 0, center[n + 1], center[n]), LANES - 1, 1)
                value = keep * center[n] + weights[0] * beside_x
                value = value + weights[1] * (low + high)
                value = value + weights[2] * (left + right)
                store(n, y, value)

    for s in range(SWEEPS - 1):
        for g, size in enumerate(GROUPS):
            wait_faces(s, g)
            if s > 0:
                wait_sent(s - 1, g)
            after = states[(s + 1) % 2]

            def one_vector(k, carry, s=s, after=after):
                def one_plane(x, carry):
                    def store(n, y, value):
                        r = n * rows_y + y
                        after[k, x, r : r + 8, :] = value

                    plane_sweep(s, k, x, store)
                    return carry

                lax.fori_loop(1, rows_x + 1, one_plane, 0, unroll=UNROLL)
                pack(s + 1, k)
                return carry

            lax.fori_loop(starts[g], starts[g] + size, one_vector, 0)
            send(s + 1, g)
            if s == 0 and 2 <= g < 2 + len(ROUNDS):
                hear(g - 2)

    half_x, half_y = rows_x // 2, rows_y // 2
    even = lax.rem(lane, 2) == 0
    part = zero
    s = SWEEPS - 1

    def add_products(part, k, first, sums):
        stacked = zero
        for other in range(k + 1):
            summed = jnp.sum(sums[other], axis=0, keepdims=True)
            stacked = jnp.where(row == other, summed, stacked)
        column = jnp.broadcast_to(jnp.sum(stacked, axis=1, keepdims=True), (8, LANES))
        across = jnp.sum(jnp.where(lane == row + first, column, 0.0), axis=0, keepdims=True)
        part = jnp.where((lane == first + k) & (row <= k), column, part)
        inside = (row == k) & (lane >= first) & (lane < first + k)
        return jnp.where(inside, jnp.broadcast_to(across, (8, LANES)), part)

    for k in range(K):
        if k in starts:
            wait_faces(s, starts.index(k))

        def last_plane(x, sums):
            fine = list(sums)

            def store(n, y, value):
                window = (x - 1, slice(y, y + 8), slice((n - 1) * LANES, n * LANES))
                fields_ref[(k, *window)] = value
                for other in range(k):
                    fine[other] = fine[other] + value * fields_ref[(other, *window)]
                fine[k] = fine[k] + value * value

            plane_sweep(s, k, x, store)
            return tuple(fine)

        fine = lax.fori_loop(1, rows_x + 1, last_plane, (zero,) * (k + 1), unroll=UNROLL_LAST)

        part = add_products(part, k, 0, fine)

        def aggregate(i, sums):
            rest = list(sums)
            for n in range(blocks):
                columns = slice(n * LANES, (n + 1) * LANES)
                for y in range(0, rows_y, 8):
                    pairs[n, y : y + 8, :] = (
                        fields_ref[k, 2 * i, y : y + 8, columns]
                        + fields_ref[k, 2 * i + 1, y : y + 8, columns]
                    )
            for n in range(blocks):
                value = (
                    pairs[n, pl.ds(0, half_y, stride=2), :]
                    + pairs[n, pl.ds(1, half_y, stride=2), :]
                )
                value = 0.125 * (value + pltpu.roll(value, LANES - 1, 1))
                value = jnp.where(even, value, 0.0)
                sums_z[k, i, n] = value
                for other in range(k):
                    rest[other] = rest[other] + value * sums_z[other, i, n]
                rest[k] = rest[k] + value * value
            return tuple(rest)

        rest = lax.fori_loop(0, half_x, aggregate, (zero,) * (k + 1), unroll=UNROLL_HALF)
        part = add_products(part, k, K, rest)

    def pack_lanes(k, carry):
        index = lax.rem(2 * lane, LANES)
        for i in range(half_x):
            for n in range(0, blocks, 2):
                low = jnp.take_along_axis(sums_z[k, i, n], index, axis=1)
                high = jnp.take_along_axis(sums_z[k, i, n + 1], index, axis=1)
                window = (i, slice(None), slice(n // 2 * LANES, (n // 2 + 1) * LANES))
                coarse_ref[(k, *window)] = jnp.where(lane < LANES // 2, low, high)
        return carry

    stages = (
        (NEAR, gather_near, near_send, near_recv),
        (FAR, gather_far, far_send, far_recv),
    )
    for stage, (axes, slots, sent, received) in enumerate(stages):
        me = slot_of(sizes, position, axes)
        group = others(sizes, axes)
        slots[me] = part

        def exchange(number, axes=axes, slots=slots, me=me, group=group, sent=sent, received=received):
            return pltpu.make_async_remote_copy(
                src_ref=slots.at[me],
                dst_ref=slots.at[me],
                send_sem=sent.at[number],
                recv_sem=received.at[number],
                device_id=shifted(sizes, position, axes, group[number]),
                device_id_type=MESH,
            )

        def arrival(number, axes=axes, slots=slots, group=group, sent=sent, received=received):
            back = tuple(sizes[a] - o for a, o in zip(axes, group[number]))
            where = shifted(sizes, position, axes, back)
            source = slot_of(sizes, where, axes)
            return pltpu.make_async_remote_copy(
                src_ref=slots.at[source],
                dst_ref=slots.at[source],
                send_sem=sent.at[number],
                recv_sem=received.at[number],
                device_id=where,
                device_id_type=MESH,
            )

        for number in range(len(group)):
            exchange(number).start()
        half = K // 2
        lax.fori_loop(stage * half, (stage + 1) * half, pack_lanes, 0)
        for number in range(len(group)):
            arrival(number).wait_recv()
        part = slots[0]
        for slot in range(1, len(group) + 1):
            part = part + slots[slot]
        for number in range(len(group)):
            exchange(number).wait_send()
    gram_ref[...] = part

    for s in range(SWEEPS - 2, SWEEPS):
        for g in range(len(GROUPS)):
            wait_sent(s, g)


def inverse_factor(entry):
    left = {(k, j): entry(k, j) for k in range(K) for j in range(k + 1)}
    factor, inverse, scale = {}, {}, []
    for j in range(K):
        scale.append(lax.rsqrt(left[j, j]))
        reciprocal = 1.0 / left[j, j]
        for k in range(j + 1, K):
            factor[k, j] = left[k, j] * reciprocal
        for k in range(j + 1, K):
            for other in range(j + 1, k + 1):
                left[k, other] = left[k, other] - factor[k, j] * left[other, j]
    for k in range(K):
        for j in range(k):
            total = factor[k, j]
            for other in range(j + 1, k):
                total = total + factor[k, other] * inverse[other, j]
            inverse[k, j] = -total
    result = {(k, j): scale[k] * inverse[k, j] for k in range(K) for j in range(k)}
    result.update({(k, k): scale[k] for k in range(K)})
    return result


def basis_kernel(
    cells,
    gram_ref,
    fields_ref,
    coarse_ref,
    basis_ref,
    coarse_basis_ref,
    stage,
    coarse_stage,
    columns,
    table,
    out_sem,
    coarse_sem,
):
    rows_x, rows_y, blocks = (
        fields_ref.shape[1],
        fields_ref.shape[2],
        fields_ref.shape[3] // LANES,
    )
    gram = gram_ref[...]
    for which, count in enumerate((cells, cells // 8)):
        mean = gram / count
        for j in range(K):
            c = which * K + j
            columns[c] = jnp.broadcast_to(mean[:, c : c + 1], (8, LANES))
    for which in range(2):

        def entry(k, j, which=which):
            return jnp.broadcast_to(columns[which * K + j, k : k + 1, :], (8, LANES))

        for (k, j), value in inverse_factor(entry).items():
            table[which, k * (k + 1) // 2 + j] = value

    def combine(which, windows, source, target):
        loaded = [[source(other, w) for w in windows] for other in range(K)]
        for k in range(K):
            totals = None
            for other in range(k + 1):
                weight = table[which, k * (k + 1) // 2 + other]
                products = [weight * value for value in loaded[other]]
                totals = (
                    products if totals is None else [t + p for t, p in zip(totals, products)]
                )
            for w, total in zip(windows, totals):
                target(k, w, total)

    def put(x):
        return pltpu.make_async_copy(stage.at[x], basis_ref.at[:, x], out_sem.at[x])

    def one_plane(x, carry):
        def source(k, w):
            return fields_ref[k, x, w[0] : w[0] + 8, w[1] * LANES : (w[1] + 1) * LANES]

        def target(k, w, value):
            stage[x, k, w[0] : w[0] + 8, w[1] * LANES : (w[1] + 1) * LANES] = value

        windows = [(y, n) for y in range(0, rows_y, 8) for n in range(blocks)]
        for first in range(0, len(windows), 4):
            combine(0, windows[first : first + 4], source, target)
        put(x).start()
        return carry

    def one_coarse(x, carry):
        def source(k, n):
            return coarse_ref[k, x, :, n * LANES : (n + 1) * LANES]

        def target(k, n, value):
            coarse_stage[k, x, :, n * LANES : (n + 1) * LANES] = value

        combine(1, list(range(blocks // 2)), source, target)
        return carry

    lax.fori_loop(0, rows_x // 2, one_plane, 0)
    lax.fori_loop(0, rows_x // 2, one_coarse, 0)
    out = pltpu.make_async_copy(coarse_stage, coarse_basis_ref, coarse_sem)
    out.start()
    lax.fori_loop(rows_x // 2, rows_x, one_plane, 0)

    def drain(x, carry):
        put(x).wait()
        return carry

    lax.fori_loop(0, rows_x, drain, 0)
    out.wait()


def local(sizes, test_vectors, aniso):
    vectors, rows_x, rows_y, rows_z = test_vectors.shape
    blocks = rows_z // LANES
    half = (vectors, rows_x // 2, rows_y // 2, rows_z // 2)
    f32 = jnp.float32
    hbm = pl.BlockSpec(memory_space=pltpu.HBM)
    vmem = pl.BlockSpec(memory_space=pltpu.VMEM)
    near, far = len(others(sizes, NEAR)), len(others(sizes, FAR))
    fields, coarse, gram = pl.pallas_call(
        functools.partial(sweep_kernel, sizes),
        out_shape=(
            pltpu.VMEM(test_vectors.shape, f32),
            pltpu.VMEM(half, f32),
            pltpu.VMEM((8, LANES), f32),
        ),
        in_specs=[hbm, hbm],
        out_specs=(vmem, vmem, vmem),
        scratch_shapes=[
            pltpu.SMEM(aniso.shape[::-1], jnp.int32),
            pltpu.VMEM((vectors, rows_x + 2, (blocks + 2) * rows_y, LANES), f32),
            pltpu.VMEM((vectors, rows_x + 2, (blocks + 2) * rows_y, LANES), f32),
            pltpu.VMEM((SWEEPS, 2, vectors, rows_x, blocks, LANES), f32),
            pltpu.VMEM((SWEEPS, 2, vectors, rows_x, blocks, LANES), f32),
            pltpu.VMEM((blocks, rows_y, LANES), f32),
            pltpu.VMEM((vectors, rows_x // 2, blocks, rows_y // 2, LANES), f32),
            pltpu.VMEM((near + 1, 8, LANES), f32),
            pltpu.VMEM((far + 1, 8, LANES), f32),
            pltpu.SemaphoreType.DMA(()),
            pltpu.SemaphoreType.DMA((vectors, blocks)),
            pltpu.SemaphoreType.DMA((6, SWEEPS, len(GROUPS))),
            pltpu.SemaphoreType.DMA((6, SWEEPS, len(GROUPS))),
            pltpu.SemaphoreType.DMA((near,)),
            pltpu.SemaphoreType.DMA((near,)),
            pltpu.SemaphoreType.DMA((far,)),
            pltpu.SemaphoreType.DMA((far,)),
            pltpu.SemaphoreType.REGULAR((len(ROUNDS),)),
        ],
        compiler_params=pltpu.CompilerParams(
            collective_id=0, has_side_effects=True, vmem_limit_bytes=44 * 1024 * 1024
        ),
        name="sweeps",
    )(pltpu.with_memory_space_constraint(aniso.T, pltpu.HBM), test_vectors)
    cells = float(rows_x * rows_y * rows_z * sizes["gx"] * sizes["gy"] * sizes["gz"])
    return pl.pallas_call(
        functools.partial(basis_kernel, cells),
        out_shape=(
            jax.ShapeDtypeStruct(test_vectors.shape, f32),
            jax.ShapeDtypeStruct(half, f32),
        ),
        in_specs=[vmem, vmem, vmem],
        out_specs=(hbm, hbm),
        scratch_shapes=[
            pltpu.VMEM((rows_x, vectors, rows_y, rows_z), f32),
            pltpu.VMEM(half, f32),
            pltpu.VMEM((2 * vectors, 8, LANES), f32),
            pltpu.VMEM((2, vectors * (vectors + 1) // 2, 8, LANES), f32),
            pltpu.SemaphoreType.DMA((rows_x,)),
            pltpu.SemaphoreType.DMA(()),
        ],
        compiler_params=pltpu.CompilerParams(vmem_limit_bytes=24 * 1024 * 1024),
        name="basis",
    )(gram, fields, coarse)


def solution(mesh):
    sizes = {axis: mesh.shape[axis] for axis in AXES}
    spec = P(None, "gx", "gy", "gz")
    return jax.shard_map(
        functools.partial(local, sizes),
        mesh=mesh,
        in_specs=(spec, P()),
        out_specs=(spec, spec),
        check_vma=False,
    )
```

```python
import functools
import itertools

import jax
import jax.numpy as jnp
from jax import lax
from jax.experimental import pallas as pl
from jax.experimental.pallas import tpu as pltpu
from jax.sharding import PartitionSpec as P

MESH = pl.DeviceIdType.MESH
omega_weight = 2.0 / 3.0
K = 8
SWEEPS = 3
LANES = 128
AXES = ("gx", "gy", "gz")
UNROLL = 8
GROUPS = (1,) * 8
UNROLL_LAST = 8
UNROLL_HALF = 4


NEAR = ("gz",)
FAR = ("gx", "gy")
ROUNDS = (
    (("gz", 1), ("gx", 1)),
    (("gz", 2), ("gx", 2)),
    (("gz", 4), ("gy", 1)),
    (("gy", 1),),
    (("gy", 2),),
)


def others(sizes, axes):
    return [o for o in itertools.product(*(range(sizes[a]) for a in axes)) if any(o)]


def shifted(sizes, position, axes, offsets):
    return {a: lax.rem(position[a] + o, sizes[a]) for a, o in zip(axes, offsets)}


def slot_of(sizes, where, axes):
    slot = 0
    for axis in axes:
        slot = slot * sizes[axis] + where[axis]
    return slot


def sweep_kernel(
    sizes,
    aniso_hbm,
    in_ref,
    fields_ref,
    coarse_ref,
    gram_ref,
    aniso_ref,
    even_state,
    odd_state,
    ysend,
    yrecv,
    pairs,
    sums_z,
    gather_near,
    gather_far,
    aniso_sem,
    load_sem,
    send_sem,
    recv_sem,
    near_send,
    near_recv,
    far_send,
    far_recv,
    rounds,
):
    rows_x, rows_y, blocks = (in_ref.shape[1], in_ref.shape[2], in_ref.shape[3] // LANES)
    area = blocks * rows_y
    states = (even_state, odd_state)
    position = {axis: lax.axis_index(axis) for axis in AXES}

    def load(k, block):
        return pltpu.make_async_copy(
            in_ref.at[k, :, :, pl.ds(block * LANES, LANES)],
            even_state.at[k, pl.ds(1, rows_x), pl.ds((block + 1) * rows_y, rows_y), :],
            load_sem.at[k, block],
        )

    def start_loads(k, carry):
        for block in range(blocks):
            load(k, block).start()
        return carry

    fetch = pltpu.make_async_copy(aniso_hbm, aniso_ref, aniso_sem)
    fetch.start()
    lax.fori_loop(0, K, start_loads, 0)

    def greet(semaphore, axis, distance):
        heard = 0
        for step in (-distance, distance):
            there = position[axis] >= distance if step < 0 else position[axis] < sizes[axis] - distance

            @pl.when(there)
            def _():
                pl.semaphore_signal(
                    semaphore,
                    inc=1,
                    device_id={axis: position[axis] + step},
                    device_id_type=MESH,
                )

            heard = heard + there.astype(jnp.int32)
        return heard

    barrier = pltpu.get_barrier_semaphore()
    peers = sum(greet(barrier, axis, 1) for axis in AXES)

    def hear(number):
        heard = sum(greet(rounds.at[number], axis, d) for axis, d in ROUNDS[number])
        pl.semaphore_wait(rounds.at[number], heard)

    lane = lax.broadcasted_iota(jnp.int32, (8, LANES), 1)
    row = lax.broadcasted_iota(jnp.int32, (8, LANES), 0)

    starts = [sum(GROUPS[:g]) for g in range(len(GROUPS))]

    def face(s, g, direction):
        vectors = pl.ds(starts[g], GROUPS[g])
        state = states[s % 2]
        axis, side = AXES[direction // 2], direction % 2
        peer = position[axis] + (1 if side else -1)
        if axis == "gx":
            source = state.at[vectors, rows_x if side else 1, pl.ds(rows_y, area), :]
            target = state.at[vectors, 0 if side else rows_x + 1, pl.ds(rows_y, area), :]
        elif axis == "gy":
            source = ysend.at[s, side, vectors]
            target = yrecv.at[s, side, vectors]
        else:
            from_row = blocks * rows_y if side else rows_y
            to_row = 0 if side else (blocks + 1) * rows_y
            source = state.at[vectors, pl.ds(1, rows_x), pl.ds(from_row, rows_y), :]
            target = state.at[vectors, pl.ds(1, rows_x), pl.ds(to_row, rows_y), :]
        return pltpu.make_async_remote_copy(
            src_ref=source,
            dst_ref=target,
            send_sem=send_sem.at[direction, s, g],
            recv_sem=recv_sem.at[direction, s, g],
            device_id={axis: peer},
            device_id_type=MESH,
        )

    def can_send(direction):
        axis, side = AXES[direction // 2], direction % 2
        return position[axis] < sizes[axis] - 1 if side else position[axis] > 0

    def can_receive(direction):
        return can_send(direction ^ 1)

    def pack(s, k):
        state = states[s % 2]

        def pack_plane(x, carry):
            for side in range(2):
                first = rows_y + (rows_y - 1 if side else 0)
                ysend[s, side, k, x] = state[k, x + 1, pl.ds(first, blocks, stride=rows_y), :]
            return carry

        lax.fori_loop(0, rows_x, pack_plane, 0, unroll=4)

    def send(s, g):
        for direction in range(6):

            @pl.when(can_send(direction))
            def _():
                face(s, g, direction).start()

    def wait_faces(s, g):
        for direction in range(6):

            @pl.when(can_receive(direction))
            def _():
                face(s, g, direction).wait_recv()

    def wait_sent(s, g):
        for direction in range(6):

            @pl.when(can_send(direction))
            def _():
                face(s, g, direction).wait_send()

    zero = jnp.zeros((8, LANES), jnp.float32)

    def clear(direction):
        axis, side = AXES[direction // 2], direction % 2

        def clear_one(k, carry):
            if axis == "gx":
                plane = 0 if side else rows_x + 1
                for state in states:
                    for r in range(0, area, 8):
                        state[k, plane, rows_y + r : rows_y + r + 8, :] = zero
            elif axis == "gy":
                for s in range(SWEEPS):
                    for x in range(rows_x):
                        yrecv[s, side, k, x] = zero
            else:
                first = 0 if side else (blocks + 1) * rows_y
                for state in states:
                    for x in range(rows_x):
                        for r in range(0, rows_y, 8):
                            state[k, x + 1, first + r : first + r + 8, :] = zero
            return carry

        lax.fori_loop(0, K, clear_one, 0)

    pl.semaphore_wait(barrier, peers)

    def loaded(k, carry):
        for block in range(blocks):
            load(k, block).wait()
        pack(0, k)
        return carry

    for g, size in enumerate(GROUPS):
        lax.fori_loop(starts[g], starts[g] + size, loaded, 0)
        send(0, g)

    for direction in range(6):

        @pl.when(jnp.logical_not(can_receive(direction)))
        def _():
            clear(direction)

    fetch.wait()

    def as_float(d, j):
        return jnp.full((8, LANES), aniso_ref[j, d], jnp.int32).astype(jnp.float32)

    coefficients = [as_float(d, 0) / as_float(d, 1) for d in range(3)]
    scaled = omega_weight / (2.0 * (coefficients[0] + coefficients[1] + coefficients[2]))
    weights = [scaled * c for c in coefficients]
    keep = 1.0 - omega_weight

    def plane_sweep(s, k, x, store):
        state = states[s % 2]
        for y in range(0, rows_y, 8):
            center = [
                state[k, x, n * rows_y + y : n * rows_y + y + 8, :] for n in range(blocks + 2)
            ]
            for n in range(1, blocks + 1):
                r = n * rows_y + y
                beside_x = state[k, x - 1, r : r + 8, :] + state[k, x + 1, r : r + 8, :]
                low = state[k, x, r - 1 : r + 7, :]
                high = state[k, x, r + 1 : r + 9, :]
                if y == 0:
                    edge = jnp.broadcast_to(yrecv[s, 1, k, x - 1, n - 1 : n, :], (8, LANES))
                    low = jnp.where(row == 0, edge, low)
                if y == rows_y - 8:
                    edge = jnp.broadcast_to(yrecv[s, 0, k, x - 1, n - 1 : n, :], (8, LANES))
                    high = jnp.where(row == 7, edge, high)
                left = pltpu.roll(jnp.where(lane == LANES - 1, center[n - 1], center[n]), 1, 1)
                right = pltpu.roll(jnp.where(lane == 0, center[n + 1], center[n]), LANES - 1, 1)
                value = keep * center[n] + weights[0] * beside_x
                value = value + weights[1] * (low + high)
                value = value + weights[2] * (left + right)
                store(n, y, value)

    for s in range(SWEEPS - 1):
        for g, size in enumerate(GROUPS):
            wait_faces(s, g)
            if s > 0:
                wait_sent(s - 1, g)
            after = states[(s + 1) % 2]

            def one_vector(k, carry, s=s, after=after):
                def one_plane(x, carry):
                    def store(n, y, value):
                        r = n * rows_y + y
                        after[k, x, r : r + 8, :] = value

                    plane_sweep(s, k, x, store)
                    return carry

                lax.fori_loop(1, rows_x + 1, one_plane, 0, unroll=UNROLL)
                pack(s + 1, k)
                return carry

            lax.fori_loop(starts[g], starts[g] + size, one_vector, 0)
            send(s + 1, g)
            if s == 0 and 2 <= g < 2 + len(ROUNDS):
                hear(g - 2)

    half_x, half_y = rows_x // 2, rows_y // 2
    even = lax.rem(lane, 2) == 0
    part = zero
    s = SWEEPS - 1

    def add_products(part, k, first, sums):
        stacked = zero
        for other in range(k + 1):
            summed = jnp.sum(sums[other], axis=0, keepdims=True)
            stacked = jnp.where(row == other, summed, stacked)
        column = jnp.broadcast_to(jnp.sum(stacked, axis=1, keepdims=True), (8, LANES))
        across = jnp.sum(jnp.where(lane == row + first, column, 0.0), axis=0, keepdims=True)
        part = jnp.where((lane == first + k) & (row <= k), column, part)
        inside = (row == k) & (lane >= first) & (lane < first + k)
        return jnp.where(inside, jnp.broadcast_to(across, (8, LANES)), part)

    for k in range(K):
        if k in starts:
            wait_faces(s, starts.index(k))

        def last_plane(x, sums):
            fine = list(sums)

            def store(n, y, value):
                window = (x - 1, slice(y, y + 8), slice((n - 1) * LANES, n * LANES))
                fields_ref[(k, *window)] = value
                for other in range(k):
                    fine[other] = fine[other] + value * fields_ref[(other, *window)]
                fine[k] = fine[k] + value * value

            plane_sweep(s, k, x, store)
            return tuple(fine)

        fine = lax.fori_loop(1, rows_x + 1, last_plane, (zero,) * (k + 1), unroll=UNROLL_LAST)

        part = add_products(part, k, 0, fine)

        def aggregate(i, sums):
            rest = list(sums)
            for n in range(blocks):
                columns = slice(n * LANES, (n + 1) * LANES)
                for y in range(0, rows_y, 8):
                    pairs[n, y : y + 8, :] = (
                        fields_ref[k, 2 * i, y : y + 8, columns]
                        + fields_ref[k, 2 * i + 1, y : y + 8, columns]
                    )
            for n in range(blocks):
                value = (
                    pairs[n, pl.ds(0, half_y, stride=2), :]
                    + pairs[n, pl.ds(1, half_y, stride=2), :]
                )
                value = 0.125 * (value + pltpu.roll(value, LANES - 1, 1))
                value = jnp.where(even, value, 0.0)
                sums_z[k, i, n] = value
                for other in range(k):
                    rest[other] = rest[other] + value * sums_z[other, i, n]
                rest[k] = rest[k] + value * value
            return tuple(rest)

        rest = lax.fori_loop(0, half_x, aggregate, (zero,) * (k + 1), unroll=UNROLL_HALF)
        part = add_products(part, k, K, rest)

    def pack_lanes(k, carry):
        index = lax.rem(2 * lane, LANES)
        for i in range(half_x):
            for n in range(0, blocks, 2):
                low = jnp.take_along_axis(sums_z[k, i, n], index, axis=1)
                high = jnp.take_along_axis(sums_z[k, i, n + 1], index, axis=1)
                window = (i, slice(None), slice(n // 2 * LANES, (n // 2 + 1) * LANES))
                coarse_ref[(k, *window)] = jnp.where(lane < LANES // 2, low, high)
        return carry

    stages = (
        (NEAR, gather_near, near_send, near_recv),
        (FAR, gather_far, far_send, far_recv),
    )
    for stage, (axes, slots, sent, received) in enumerate(stages):
        me = slot_of(sizes, position, axes)
        group = others(sizes, axes)
        slots[me] = part

        def exchange(number, axes=axes, slots=slots, me=me, group=group, sent=sent, received=received):
            return pltpu.make_async_remote_copy(
                src_ref=slots.at[me],
                dst_ref=slots.at[me],
                send_sem=sent.at[number],
                recv_sem=received.at[number],
                device_id=shifted(sizes, position, axes, group[number]),
                device_id_type=MESH,
            )

        def arrival(number, axes=axes, slots=slots, group=group, sent=sent, received=received):
            back = tuple(sizes[a] - o for a, o in zip(axes, group[number]))
            where = shifted(sizes, position, axes, back)
            source = slot_of(sizes, where, axes)
            return pltpu.make_async_remote_copy(
                src_ref=slots.at[source],
                dst_ref=slots.at[source],
                send_sem=sent.at[number],
                recv_sem=received.at[number],
                device_id=where,
                device_id_type=MESH,
            )

        for number in range(len(group)):
            exchange(number).start()
        half = K // 2
        lax.fori_loop(stage * half, (stage + 1) * half, pack_lanes, 0)
        for g in range(len(GROUPS)):
            wait_sent(SWEEPS - 2 + stage, g)
        for number in range(len(group)):
            arrival(number).wait_recv()
        part = slots[0]
        for slot in range(1, len(group) + 1):
            part = part + slots[slot]
        for number in range(len(group)):
            exchange(number).wait_send()
    gram_ref[...] = part


def inverse_factor(entry):
    left = {(k, j): entry(k, j) for k in range(K) for j in range(k + 1)}
    factor, inverse, scale = {}, {}, []
    for j in range(K):
        scale.append(lax.rsqrt(left[j, j]))
        reciprocal = 1.0 / left[j, j]
        for k in range(j + 1, K):
            factor[k, j] = left[k, j] * reciprocal
        for k in range(j + 1, K):
            for other in range(j + 1, k + 1):
                left[k, other] = left[k, other] - factor[k, j] * left[other, j]
    for k in range(K):
        for j in range(k):
            total = factor[k, j]
            for other in range(j + 1, k):
                total = total + factor[k, other] * inverse[other, j]
            inverse[k, j] = -total
    result = {(k, j): scale[k] * inverse[k, j] for k in range(K) for j in range(k)}
    result.update({(k, k): scale[k] for k in range(K)})
    return result


def basis_kernel(
    cells,
    gram_ref,
    fields_ref,
    coarse_ref,
    basis_ref,
    coarse_basis_ref,
    stage,
    coarse_stage,
    columns,
    table,
    out_sem,
    coarse_sem,
):
    rows_x, rows_y, blocks = (
        fields_ref.shape[1],
        fields_ref.shape[2],
        fields_ref.shape[3] // LANES,
    )
    gram = gram_ref[...]
    for which, count in enumerate((cells, cells // 8)):
        mean = gram / count
        for j in range(K):
            c = which * K + j
            columns[c] = jnp.broadcast_to(mean[:, c : c + 1], (8, LANES))
    for which in range(2):

        def entry(k, j, which=which):
            return jnp.broadcast_to(columns[which * K + j, k : k + 1, :], (8, LANES))

        for (k, j), value in inverse_factor(entry).items():
            table[which, k * (k + 1) // 2 + j] = value

    def combine(which, windows, source, target):
        loaded = [[source(other, w) for w in windows] for other in range(K)]
        for k in range(K):
            totals = None
            for other in range(k + 1):
                weight = table[which, k * (k + 1) // 2 + other]
                products = [weight * value for value in loaded[other]]
                totals = (
                    products if totals is None else [t + p for t, p in zip(totals, products)]
                )
            for w, total in zip(windows, totals):
                target(k, w, total)

    def put(x):
        return pltpu.make_async_copy(stage.at[x], basis_ref.at[:, x], out_sem.at[x])

    def one_plane(x, carry):
        def source(k, w):
            return fields_ref[k, x, w[0] : w[0] + 8, w[1] * LANES : (w[1] + 1) * LANES]

        def target(k, w, value):
            stage[x, k, w[0] : w[0] + 8, w[1] * LANES : (w[1] + 1) * LANES] = value

        windows = [(y, n) for y in range(0, rows_y, 8) for n in range(blocks)]
        for first in range(0, len(windows), 4):
            combine(0, windows[first : first + 4], source, target)
        put(x).start()
        return carry

    def one_coarse(x, carry):
        def source(k, n):
            return coarse_ref[k, x, :, n * LANES : (n + 1) * LANES]

        def target(k, n, value):
            coarse_stage[k, x, :, n * LANES : (n + 1) * LANES] = value

        combine(1, list(range(blocks // 2)), source, target)
        return carry

    lax.fori_loop(0, rows_x // 2, one_plane, 0)
    lax.fori_loop(0, rows_x // 2, one_coarse, 0)
    out = pltpu.make_async_copy(coarse_stage, coarse_basis_ref, coarse_sem)
    out.start()
    lax.fori_loop(rows_x // 2, rows_x, one_plane, 0)

    def drain(x, carry):
        put(x).wait()
        return carry

    lax.fori_loop(0, rows_x, drain, 0)
    out.wait()


def local(sizes, test_vectors, aniso):
    vectors, rows_x, rows_y, rows_z = test_vectors.shape
    blocks = rows_z // LANES
    half = (vectors, rows_x // 2, rows_y // 2, rows_z // 2)
    f32 = jnp.float32
    hbm = pl.BlockSpec(memory_space=pltpu.HBM)
    vmem = pl.BlockSpec(memory_space=pltpu.VMEM)
    near, far = len(others(sizes, NEAR)), len(others(sizes, FAR))
    fields, coarse, gram = pl.pallas_call(
        functools.partial(sweep_kernel, sizes),
        out_shape=(
            pltpu.VMEM(test_vectors.shape, f32),
            pltpu.VMEM(half, f32),
            pltpu.VMEM((8, LANES), f32),
        ),
        in_specs=[hbm, hbm],
        out_specs=(vmem, vmem, vmem),
        scratch_shapes=[
            pltpu.SMEM(aniso.shape[::-1], jnp.int32),
            pltpu.VMEM((vectors, rows_x + 2, (blocks + 2) * rows_y, LANES), f32),
            pltpu.VMEM((vectors, rows_x + 2, (blocks + 2) * rows_y, LANES), f32),
            pltpu.VMEM((SWEEPS, 2, vectors, rows_x, blocks, LANES), f32),
            pltpu.VMEM((SWEEPS, 2, vectors, rows_x, blocks, LANES), f32),
            pltpu.VMEM((blocks, rows_y, LANES), f32),
            pltpu.VMEM((vectors, rows_x // 2, blocks, rows_y // 2, LANES), f32),
            pltpu.VMEM((near + 1, 8, LANES), f32),
            pltpu.VMEM((far + 1, 8, LANES), f32),
            pltpu.SemaphoreType.DMA(()),
            pltpu.SemaphoreType.DMA((vectors, blocks)),
            pltpu.SemaphoreType.DMA((6, SWEEPS, len(GROUPS))),
            pltpu.SemaphoreType.DMA((6, SWEEPS, len(GROUPS))),
            pltpu.SemaphoreType.DMA((near,)),
            pltpu.SemaphoreType.DMA((near,)),
            pltpu.SemaphoreType.DMA((far,)),
            pltpu.SemaphoreType.DMA((far,)),
            pltpu.SemaphoreType.REGULAR((len(ROUNDS),)),
        ],
        compiler_params=pltpu.CompilerParams(
            collective_id=0, has_side_effects=True, vmem_limit_bytes=44 * 1024 * 1024
        ),
        name="sweeps",
    )(pltpu.with_memory_space_constraint(aniso.T, pltpu.HBM), test_vectors)
    cells = float(rows_x * rows_y * rows_z * sizes["gx"] * sizes["gy"] * sizes["gz"])
    return pl.pallas_call(
        functools.partial(basis_kernel, cells),
        out_shape=(
            jax.ShapeDtypeStruct(test_vectors.shape, f32),
            jax.ShapeDtypeStruct(half, f32),
        ),
        in_specs=[vmem, vmem, vmem],
        out_specs=(hbm, hbm),
        scratch_shapes=[
            pltpu.VMEM((rows_x, vectors, rows_y, rows_z), f32),
            pltpu.VMEM(half, f32),
            pltpu.VMEM((2 * vectors, 8, LANES), f32),
            pltpu.VMEM((2, vectors * (vectors + 1) // 2, 8, LANES), f32),
            pltpu.SemaphoreType.DMA((rows_x,)),
            pltpu.SemaphoreType.DMA(()),
        ],
        compiler_params=pltpu.CompilerParams(vmem_limit_bytes=24 * 1024 * 1024),
        name="basis",
    )(gram, fields, coarse)


def solution(mesh):
    sizes = {axis: mesh.shape[axis] for axis in AXES}
    spec = P(None, "gx", "gy", "gz")
    return jax.shard_map(
        functools.partial(local, sizes),
        mesh=mesh,
        in_specs=(spec, P()),
        out_specs=(spec, spec),
        check_vma=False,
    )
```
